32 devices in a mesh: dp: 8 (over z, x), expert: 4 (over y, core).
Axes of the slice: x: 2, y: 2, z: 4, core: 2. Of those that a mesh axis runs over, the one named last changes fastest.
Arguments:
- tokens: bfloat16 [2, 8192, 1024], P(None, ('dp', 'expert')), may hold values from -6 to 6
- lengths: int32 [2, 8], P(None, 'dp'), may hold values from 256 to 1024, as said below
- routes: int32 [2, 8192, 2], P(None, ('dp', 'expert')), may hold values from 0 to 3, all different within a row
- w_qkv: bfloat16 [1024, 3072], P(('dp', 'expert')), may hold values from -0.1875 to 0.1875
- w_out: bfloat16 [1024, 1024], P(('dp', 'expert')), may hold values from -3 to 3
- norm_gains: bfloat16 [1024, 2], P(('dp', 'expert')), may hold values from 0.5 to 1.5
- bias_table: bfloat16 [512], P(('dp', 'expert')), may hold values from -4 to 4
- router: bfloat16 [1024, 4], P(('dp', 'expert')), may hold values from -0.09375 to 0.09375
- w_in: bfloat16 [4, 1024, 5632], P('expert', 'dp'), may hold values from -0.1875 to 0.1875
- w_down: bfloat16 [4, 2816, 1024], P('expert', 'dp'), may hold values from -0.4375 to 0.4375
- cotangent: bfloat16 [2, 8192, 1024], P(None, ('dp', 'expert')), may hold values from -6 to 6
Outputs:
- block_out: bfloat16 [2, 8192, 1024], P(None, ('dp', 'expert'))
- grad_tokens: float32 [2, 8192, 1024], P(None, ('dp', 'expert'))
- grad_qkv: float32 [1024, 3072], P(('dp', 'expert'))
- grad_out_proj: float32 [1024, 1024], P(('dp', 'expert'))
- grad_gains: float32 [1024, 2], P(('dp', 'expert'))
- grad_bias: float32 [512], P(('dp', 'expert'))
- grad_router: float32 [1024, 4], P(('dp', 'expert'))
- grad_w_in: float32 [4, 1024, 5632], P('expert', 'dp')
- grad_w_down: float32 [4, 2816, 1024], P('expert', 'dp')
The draws below stay inside these ranges and needn't reach their ends.
Inputs may be any that keep to these rules, and one draw needn't show every extreme that they name: `lengths`: each sequence has at least 256 live tokens; some sequence is exactly 1024 long.
All inputs are finite; a program needn't handle non-finite values.
Results may differ from the reference program's by a relative error of at most 0.02.
Values may be sent and summed in bfloat16 or wider, within the bound.
A program may use at most 320 MiB of HBM per device.

```python
import jax
import jax.numpy as jnp
from jax import lax

D = 1024
H = 16
DH = 64
FF = 2816
BUCKETS = 32
TOP = 2
LEN = 1024
MICRO = 2
EXPERTS = 4
CAP = 160
SEQS = 8


def draw_lengths(key, part):
    first, second = jax.random.split(jax.random.fold_in(key, 17))
    values = jax.random.randint(first, (MICRO, SEQS), LEN // 4, LEN + 1, dtype=jnp.int32)
    chosen = jax.random.randint(second, (), 0, MICRO * SEQS, dtype=jnp.int32)
    flat_index = jnp.arange(MICRO * SEQS, dtype=jnp.int32).reshape(MICRO, SEQS)
    values = jnp.where(flat_index == chosen, LEN, values)
    other = (chosen + 1) % (MICRO * SEQS)
    return jnp.where(flat_index == other, LEN // 4, values)


def block_levels(rng, extent, cuts, low, high):
    level, own = 1.0, jax.random.fold_in(rng, 6)
    for position, shards_of in cuts:
        draws = jnp.exp(jax.random.uniform(jax.random.fold_in(own, position), (shards_of,), jnp.float32, low / len(cuts), high / len(cuts)))
        level = level * jnp.repeat(draws, extent[position] // shards_of).reshape([-1 if axis == position else 1 for axis in range(len(extent))])
    return level


def different_ones(own_key, rows, amount, top, lift):
    order = jax.random.permutation(jax.random.fold_in(own_key, 1), amount)
    favour = order
    for power in range(3):
        favour = favour * favour // amount
    favour = favour * lift // amount
    chance = jax.random.randint(jax.random.fold_in(own_key, 2), (rows, amount), 0, 4096) + favour
    fixed_rows = jax.random.permutation(jax.random.fold_in(own_key, 3), rows)[jnp.arange(amount) % rows]
    chance = jnp.where(jnp.arange(rows)[:, None] == fixed_rows[None, :], 1 << 14, chance)
    merit = chance * amount + jnp.arange(amount)
    return lax.top_k(merit.astype(jnp.int32), top)[1].astype(jnp.int32)


def noise(stream_key, dims, spread, reach, cuts=(), kind=jnp.bfloat16):
    values = jax.random.normal(stream_key, dims, jnp.float32) * spread
    if len(cuts) > 0:
        values = block_levels(stream_key, dims, cuts, -0.22, 0.18) * values
    return jnp.clip(values, min=-reach, max=reach).astype(kind)


def setup_inputs(seed: int = 0) -> dict:
    key_list = jax.random.split(jax.random.key(seed), 12)
    return {
        "tokens": noise(key_list[0], (MICRO, SEQS * LEN, D), 1.0, 6.0, ((1, 32),)),
        "lengths": draw_lengths(jax.random.fold_in(key_list[11], 71), 0),
        "routes": different_ones(key_list[2], MICRO * (SEQS * LEN), EXPERTS, TOP, 4096).reshape((MICRO, SEQS * LEN, TOP)),
        "w_qkv": noise(key_list[3], (D, 3 * D), D ** -0.5, 0.1875, ((0, 32),)),
        "w_out": noise(key_list[4], (D, D), (D // 256) ** -0.5, 3.0, ((0, 32),)),
        "norm_gains": jnp.clip(1.0 + 0.1 * jax.random.normal(key_list[5], (D, 2), jnp.float32), 0.5, 1.5).astype(jnp.bfloat16),
        "bias_table": noise(key_list[6], (BUCKETS * H,), 1.0, 4.0, ((0, 32),)),
        "router": noise(key_list[7], (D, EXPERTS), (4 * D) ** -0.5, 0.09375, ((0, 32),)),
        "w_in": noise(key_list[8], (EXPERTS, D, 2 * FF), D ** -0.5, 0.1875, ((0, 4), (1, 8))),
        "w_down": noise(key_list[9], (EXPERTS, FF, D), (FF // 16) ** -0.5, 0.4375, ((0, 4), (1, 8))),
        "cotangent": noise(key_list[10], (MICRO, SEQS * LEN, D), 1.0, 6.0, ((1, 32),)),
    }


@jax.custom_vjp
def low(v):
    return lax.optimization_barrier(v.astype(jnp.bfloat16)).astype(jnp.float32)

@jax.custom_vjp
def low_back(v):
    return v

def low_keep(v):
    return (low(v), None)

def low_pass(kept, grad):
    return (grad,)

def back_keep(v):
    return (v, None)

def back_low(kept, grad):
    return (low(grad),)
low.defvjp(low_keep, low_pass)
low_back.defvjp(back_keep, back_low)
bucket_edges = (12, 16, 23, 32, 46, 64, 91)
norm_eps = 1e-06
highest = lax.Precision.HIGHEST

def bucket_ids(query_pos, key_pos):
    offset = key_pos[None, :] - query_pos[:, None]
    dist = jnp.abs(offset)
    beyond = jnp.zeros_like(dist)
    for edge in bucket_edges:
        beyond = beyond + (dist >= edge).astype(jnp.int32)
    near = jnp.where(dist < 8, dist, 8 + beyond)
    return near + 16 * (offset > 0).astype(jnp.int32)

def rms_scale(values, gain):
    return values * lax.rsqrt(lax.optimization_barrier(jnp.mean(values * values, axis=-1, keepdims=True)) + norm_eps) * gain

def geglu(joined):
    half = joined.shape[-1] // 2
    return jax.nn.gelu(joined[..., :half], approximate=True) * joined[..., half:]

def slot_tables(route_rows, live, experts, capacity):
    count, top = route_rows.shape
    picks = (route_rows[:, :, None] == jnp.arange(experts, dtype=jnp.int32)[None, None, :]).astype(jnp.int32) * live[:, None, None]
    flat = picks.reshape(count * top, experts)
    before = jnp.cumsum(flat, axis=0) - flat
    place = lax.optimization_barrier(jnp.sum(before * flat, axis=1)).reshape(count, top)
    kept = (place < capacity) & (live[:, None] > 0)
    target = jnp.where(kept, route_rows * capacity + place, -1)
    columns = jnp.arange(experts * capacity, dtype=jnp.int32)
    return target[:, :, None] == columns[None, None, :]

def matmul(left, right):
    return jnp.dot(left, right, precision=highest, preferred_element_type=jnp.float32)

def sequence_block(params, x, length, route_rows):
    wqkv, wout, gains, table, route_w, win, wdown = params
    positions = jnp.arange(LEN, dtype=jnp.int32)
    scale = DH ** (-0.5)
    h1 = low(rms_scale(x, gains[:, 0]))
    qkv = matmul(h1, wqkv)
    query = low_back(low(qkv[:, :D])).reshape(LEN, H, DH)
    keys = low_back(low(qkv[:, D:2 * D])).reshape(LEN, H, DH)
    values = low_back(low(qkv[:, 2 * D:])).reshape(LEN, H, DH)
    bias = jnp.transpose(table[bucket_ids(positions, positions)], (2, 0, 1))
    scores = low_back(scale * jnp.einsum('qhd,khd->hqk', query, keys, precision=highest) + bias)
    scores = jnp.where((positions < length)[None, None, :], scores, -1e+30)
    probs = low(jax.nn.softmax(scores, axis=-1))
    attended = jnp.einsum('hqk,khd->qhd', probs, values, precision=highest).reshape(LEN, D)
    attended = low_back(low(attended))
    x_mid = x + low_back(matmul(attended, wout))
    h2 = low(rms_scale(x_mid, gains[:, 1]))
    logits = low_back(matmul(h2, route_w))
    route_probs = jax.nn.softmax(logits, axis=-1)
    experts = route_w.shape[1]
    rows = LEN // experts
    route_hot = (route_rows[:, :, None] == jnp.arange(experts, dtype=jnp.int32)[None, None, :]).astype(jnp.float32)
    gates = lax.optimization_barrier(jnp.sum(route_probs[:, None, :] * route_hot, axis=-1))
    live = (positions < length).astype(jnp.int32)
    hot = jax.vmap(lambda r, l: slot_tables(r, l, experts, CAP))(route_rows.reshape(experts, rows, TOP), live.reshape(experts, rows)).astype(jnp.float32)
    sent = low_back(jnp.einsum('gtks,gtd->gsd', hot, h2.reshape(experts, rows, D), precision=highest))
    per_expert = sent.reshape(experts, experts, CAP, D).transpose(1, 0, 2, 3).reshape(experts, experts * CAP, D)
    joined = low_back(jnp.einsum('erd,edf->erf', per_expert, win, precision=highest))
    acted = low(geglu(joined))
    produced = low_back(low(jnp.einsum('erf,efd->erd', acted, wdown, precision=highest)))
    back = produced.reshape(experts, experts, CAP, D).transpose(1, 0, 2, 3).reshape(experts, experts * CAP, D)
    picked = jnp.einsum('gtks,gsd->gtkd', hot, back, precision=highest).reshape(LEN, TOP, D)
    return x_mid + lax.optimization_barrier(jnp.sum(gates[:, :, None] * picked, axis=1))

def reference(tokens, lengths, routes, w_qkv, w_out, norm_gains, bias_table, router, w_in, w_down, cotangent):
    count = MICRO * SEQS
    params = (w_qkv.astype(jnp.float32), w_out.astype(jnp.float32), norm_gains.astype(jnp.float32), bias_table.astype(jnp.float32).reshape(BUCKETS, H), router.astype(jnp.float32), w_in.astype(jnp.float32), w_down.astype(jnp.float32))
    inputs = tokens.astype(jnp.float32).reshape(count, LEN, D)
    seq_lengths = lengths.reshape(count).astype(jnp.int32)
    seq_routes = routes.reshape(count, LEN, TOP).astype(jnp.int32)
    checked = jax.checkpoint(sequence_block)

    def forward(weights, data):
        return lax.map(lambda item: checked(weights, item[0], item[1], item[2]), (data, seq_lengths, seq_routes))
    result, pull = jax.vjp(forward, params, inputs)
    grads, grad_inputs = pull(cotangent.astype(jnp.float32).reshape(count, LEN, D))
    shape = (MICRO, SEQS * LEN, D)
    return (result.astype(jnp.bfloat16).reshape(shape), grad_inputs.reshape(shape), grads[0], grads[1], grads[2], grads[3].reshape(BUCKETS * H), grads[4], grads[5], grads[6])
```

```python
import jax
import jax.numpy as jnp
from jax import lax
from jax.experimental import pallas as pl
from jax.experimental.pallas import tpu as pltpu
from jax.sharding import PartitionSpec as P

D = 1024
H = 16
DH = 64
FF = 2816
BUCKETS = 32
TOP = 2
PAIRS = H // 2
LANES = 128

bucket_edges = (12, 16, 23, 32, 46, 64, 91)
norm_eps = 1e-06
MASKED = -1e30


def bucket_of(offset):
    dist = jnp.abs(offset)
    beyond = jnp.zeros_like(dist)
    for edge in bucket_edges:
        beyond = beyond + (dist >= edge).astype(jnp.int32)
    near = jnp.where(dist < 8, dist, 8 + beyond)
    return near + 16 * (offset > 0).astype(jnp.int32)


def rms_scale(values, gain):
    return values * lax.rsqrt(jnp.mean(values * values, axis=-1, keepdims=True) + norm_eps) * gain


def geglu(joined):
    half = joined.shape[-1] // 2
    return jax.nn.gelu(joined[..., :half], approximate=True) * joined[..., half:]


def slot_tables(route_rows, live, experts, capacity):
    count, top = route_rows.shape
    picks = (route_rows[:, :, None] == jnp.arange(experts, dtype=jnp.int32)[None, None, :]).astype(
        jnp.int32
    ) * live[:, None, None]
    flat = picks.reshape(count * top, experts)
    before = jnp.cumsum(flat, axis=0) - flat
    place = jnp.sum(before * flat, axis=1).reshape(count, top)
    kept = (place < capacity) & (live[:, None] > 0)
    return jnp.where(kept, route_rows * capacity + place, -1)


def matmul(left, right):
    return jnp.dot(left, right, preferred_element_type=jnp.float32)


def inner_rows(left, right):
    return jnp.einsum("...ti,...tj->ij", left, right, preferred_element_type=jnp.float32)


def times_trans(left, right):
    return jnp.einsum("...ti,ji->...tj", left, right, preferred_element_type=jnp.float32)


def lanes_dot(left, right):
    return lax.dot_general(
        left, right, (((1,), (1,)), ((), ())), preferred_element_type=jnp.float32
    )


def rows_dot(left, right):
    return lax.dot_general(
        left, right, (((0,), (0,)), ((), ())), preferred_element_type=jnp.float32
    )


def block_place(meta_ref, piece, part, blocks):
    place = meta_ref[2 + piece] // LANES + part - meta_ref[1] // LANES + 2
    return jnp.clip(place, 0, blocks - 1)


def attend_kernel(pieces, meta_ref, *refs):
    q_ref, kv_refs, near_ref = refs[0], refs[1 : 1 + 2 * pieces], refs[1 + 2 * pieces]
    att_ref, lse_ref, score_ref = refs[2 + 2 * pieces :]
    k_refs, v_refs = kv_refs[:pieces], kv_refs[pieces:]
    rows = q_ref.shape[0]
    blocks = near_ref.shape[1]
    length = meta_ref[0]
    query = q_ref[...]
    head_of = lax.broadcasted_iota(jnp.int32, (rows, LANES), 1) // DH
    row_head = lax.broadcasted_iota(jnp.int32, (LANES, rows), 0) // DH
    key_row = lax.broadcasted_iota(jnp.int32, (LANES, rows), 0)
    out = None
    for head in range(2):
        own = head_of == head
        query_own = jnp.where(own, query, jnp.zeros_like(query))
        top = jnp.full((1, rows), MASKED, jnp.float32)
        for piece in range(pieces):
            scores = lanes_dot(k_refs[piece][...], query_own)
            for part in range(rows // LANES):
                start = meta_ref[2 + piece] + part * LANES
                block = scores[part * LANES : (part + 1) * LANES]
                block = block + near_ref[head, block_place(meta_ref, piece, part, blocks)].astype(
                    jnp.float32
                )
                block = jnp.where(key_row < length - start, block, MASKED)
                score_ref[pl.ds(piece * rows + part * LANES, LANES), :] = block
                top = jnp.maximum(top, jnp.max(block, axis=0, keepdims=True))
        total = jnp.zeros((LANES, rows), jnp.float32)
        for piece in range(pieces):
            weights = jnp.exp(score_ref[pl.ds(piece * rows, rows), :] - top).astype(jnp.bfloat16)
            value = v_refs[piece][...]
            total = total + rows_dot(jnp.where(own, value, jnp.ones_like(value)), weights)
        other = (1 - head) * DH
        norm = total[other : other + 1]
        lse_ref[0, head : head + 1] = top + jnp.log(norm)
        scaled = total / norm
        out = scaled if out is None else jnp.where(row_head == 0, out, scaled)
    att_ref[...] = out.T.astype(jnp.bfloat16)


def attend_back_kernel(pieces, meta_ref, *refs):
    q_ref, grad_ref, att_ref, lse_ref = refs[:4]
    k_refs, v_refs = refs[4 : 4 + pieces], refs[4 + pieces : 4 + 2 * pieces]
    near_ref = refs[4 + 2 * pieces]
    dq_ref = refs[5 + 2 * pieces]
    dkv_refs = refs[6 + 2 * pieces : 6 + 3 * pieces]
    dnear_ref = refs[6 + 3 * pieces]
    rows = q_ref.shape[0]
    blocks = near_ref.shape[1]
    length = meta_ref[0]
    query = q_ref[...]
    grad = grad_ref[...]
    head_of = lax.broadcasted_iota(jnp.int32, (rows, LANES), 1) // DH
    row_head = lax.broadcasted_iota(jnp.int32, (LANES, rows), 0) // DH
    key_row = lax.broadcasted_iota(jnp.int32, (LANES, rows), 0)
    product = (grad.astype(jnp.float32) * att_ref[...].astype(jnp.float32)).T
    dnear_ref[...] = jnp.zeros_like(dnear_ref)
    zero = jnp.zeros_like(query)
    query_own = [jnp.where(head_of == head, query, zero) for head in range(2)]
    grad_own = [jnp.where(head_of == head, grad, zero) for head in range(2)]
    total = [jnp.zeros((LANES, rows), jnp.float32) for head in range(2)]
    delta = [jnp.sum(product[h * DH : (h + 1) * DH], axis=0, keepdims=True) for h in range(2)]
    for piece in range(pieces):
        keys = k_refs[piece][...]
        values = v_refs[piece][...]
        dk = jnp.zeros((rows, LANES), jnp.float32)
        dv = jnp.zeros((rows, LANES), jnp.float32)
        for head in range(2):
            scores = lanes_dot(keys, query_own[head])
            grad_probs = lanes_dot(values, grad_own[head])
            lse = lse_ref[0, head : head + 1]
            prob_parts, ds_parts = [], []
            for part in range(rows // LANES):
                start = meta_ref[2 + piece] + part * LANES
                place = block_place(meta_ref, piece, part, blocks)
                cut = slice(part * LANES, (part + 1) * LANES)
                block = scores[cut] + near_ref[head, place].astype(jnp.float32)
                block = jnp.where(key_row < length - start, block, MASKED)
                probs = jnp.exp(block - lse)
                ds = probs * (grad_probs[cut] - delta[head])
                dnear_ref[head, place] += ds
                prob_parts.append(probs.astype(jnp.bfloat16))
                ds_parts.append(ds.astype(jnp.bfloat16))
            probs_low = jnp.concatenate(prob_parts, axis=0)
            ds_low = jnp.concatenate(ds_parts, axis=0)
            dv = dv + matmul(probs_low, grad_own[head])
            dk = dk + matmul(ds_low, query_own[head])
            total[head] = total[head] + rows_dot(keys, ds_low)
        dkv_refs[piece][0] = dk.astype(jnp.bfloat16)
        dkv_refs[piece][1] = dv.astype(jnp.bfloat16)
    out = jnp.where(row_head == 0, total[0], total[1])
    dq_ref[...] = (out.T * (DH ** (-0.5))).astype(jnp.bfloat16)


def attend(meta, query, kv_pieces, near):
    rows = query.shape[0]
    pieces = len(kv_pieces)
    blocks = near.shape[1]
    spec = pl.BlockSpec((rows, LANES), lambda i, m: (0, i))
    value_spec = pl.BlockSpec((rows, LANES), lambda i, m: (0, PAIRS + i))
    near_spec = pl.BlockSpec((2, blocks, LANES, rows), lambda i, m: (i, 0, 0, 0))
    lse_spec = pl.BlockSpec((1, 2, rows), lambda i, m: (i, 0, 0))
    flops = 4 * rows * rows * pieces * D
    return pl.pallas_call(
        lambda *refs: attend_kernel(pieces, *refs),
        out_shape=(
            jax.ShapeDtypeStruct((rows, D), jnp.bfloat16),
            jax.ShapeDtypeStruct((PAIRS, 2, rows), jnp.float32),
        ),
        grid_spec=pltpu.PrefetchScalarGridSpec(
            num_scalar_prefetch=1,
            grid=(PAIRS,),
            in_specs=[spec] + [spec] * pieces + [value_spec] * pieces + [near_spec],
            out_specs=[spec, lse_spec],
            scratch_shapes=[pltpu.VMEM((rows * pieces, rows), jnp.float32)],
        ),
        cost_estimate=pl.CostEstimate(
            flops=4 * flops, bytes_accessed=16 * 2**20, transcendentals=rows * rows * pieces * H
        ),
        name="attend",
    )(meta, query, *kv_pieces, *kv_pieces, near)


def attend_back(meta, query, grad, att, lse, kv_pieces, near):
    rows = query.shape[0]
    pieces = len(kv_pieces)
    blocks = near.shape[1]
    spec = pl.BlockSpec((rows, LANES), lambda i, m: (0, i))
    value_spec = pl.BlockSpec((rows, LANES), lambda i, m: (0, PAIRS + i))
    near_spec = pl.BlockSpec((2, blocks, LANES, rows), lambda i, m: (i, 0, 0, 0))
    lse_spec = pl.BlockSpec((1, 2, rows), lambda i, m: (i, 0, 0))
    dkv_spec = pl.BlockSpec((2, rows, LANES), lambda i, m: (0, 0, i))
    flops = 10 * rows * rows * pieces * D
    return pl.pallas_call(
        lambda *refs: attend_back_kernel(pieces, *refs),
        out_shape=(
            [jax.ShapeDtypeStruct((rows, D), jnp.bfloat16)]
            + [jax.ShapeDtypeStruct((2, rows, D), jnp.bfloat16)] * pieces
            + [jax.ShapeDtypeStruct(near.shape, jnp.float32)]
        ),
        grid_spec=pltpu.PrefetchScalarGridSpec(
            num_scalar_prefetch=1,
            grid=(PAIRS,),
            in_specs=[spec, spec, spec, lse_spec]
            + [spec] * pieces
            + [value_spec] * pieces
            + [near_spec],
            out_specs=[spec] + [dkv_spec] * pieces + [near_spec],
        ),
        cost_estimate=pl.CostEstimate(
            flops=4 * flops, bytes_accessed=32 * 2**20, transcendentals=rows * rows * pieces * H
        ),
        name="attend_back",
    )(meta, query, grad, att, lse, *kv_pieces, *kv_pieces, near)


def core_swap(values, experts):
    return lax.ppermute(values, "expert", [(e, e ^ 1) for e in range(experts)])


def row_shift(values, experts, step):
    return lax.ppermute(values, "expert", [(e, (e + 2 * step) % experts) for e in range(experts)])


def spread(values, experts):
    pieces = []
    for step in range(experts // 2):
        moved = row_shift(values, experts, step) if step else values
        pieces += [moved, core_swap(moved, experts)]
    return pieces


def bring_home(parts, experts):
    total = None
    for step in range(experts // 2):
        pair = parts[2 * step].astype(jnp.float32) + core_swap(parts[2 * step + 1], experts).astype(
            jnp.float32
        )
        if step:
            pair = row_shift(pair.astype(jnp.bfloat16), experts, -step).astype(jnp.float32)
        total = pair if total is None else total + pair
    return total


def swap_slots(values, experts, capacity):
    micro = values.shape[0]
    moved = lax.all_to_all(
        values.reshape(micro, experts, capacity, D),
        "expert",
        split_axis=1,
        concat_axis=1,
        tiled=True,
    )
    return moved.reshape(micro, experts * capacity, D)


def local(
    tokens, lengths, routes, w_qkv, w_out, norm_gains, bias_table, router, w_in, w_down, cotangent
):
    micro, rows, width = tokens.shape
    experts = lax.axis_size("expert")
    here = lax.axis_index("expert")
    capacity = (5 * rows * TOP + 4 * experts - 1) // (4 * experts)
    own_rows = w_qkv.shape[0]
    own_bias = bias_table.shape[0]
    spare = LANES - 3 - experts

    packed = jnp.concatenate(
        [
            w_qkv,
            w_out,
            norm_gains,
            router,
            jnp.pad(bias_table, (0, own_rows - own_bias))[:, None],
            jnp.zeros((own_rows, spare), jnp.bfloat16),
        ],
        axis=1,
    )
    packed = lax.all_gather(packed, ("dp", "expert"), axis=0, tiled=True)
    wqkv = packed[:, : 3 * D]
    wout = packed[:, 3 * D : 4 * D]
    misc = packed[:, 4 * D :]
    gains_f = misc[:, :2].astype(jnp.float32)
    route_w = misc[:, 2 : 2 + experts]
    table = misc[:, 2 + experts].reshape(D // own_rows, own_rows)[:, :own_bias]
    table = table.reshape(BUCKETS, H)
    win = lax.all_gather(w_in, "dp", axis=1, tiled=True)[0]
    wdown = lax.all_gather(w_down, "dp", axis=1, tiled=True)[0]

    blocks = rows // LANES + 4
    block_at = jnp.arange(blocks, dtype=jnp.int32)[:, None, None] - 2
    key_at = jnp.arange(LANES, dtype=jnp.int32)[None, :, None]
    query_at = jnp.arange(rows, dtype=jnp.int32)[None, None, :]
    bucket = bucket_of(block_at * LANES + key_at - query_at).reshape(-1)
    bucket_hot = (bucket[None, :] == jnp.arange(BUCKETS, dtype=jnp.int32)[:, None]).astype(
        jnp.bfloat16
    )
    near = jnp.einsum("bh,bn->hn", table, bucket_hot, preferred_element_type=jnp.float32)
    near = near.astype(jnp.bfloat16).reshape(H, blocks, LANES, rows)

    x_rows = tokens.astype(jnp.float32)
    h1 = rms_scale(x_rows, gains_f[:, 0]).astype(jnp.bfloat16)
    qkv = matmul(h1.reshape(micro * rows, D), wqkv)
    qkv = qkv.reshape(micro, rows, 3 * D)
    query = (qkv[..., :D].astype(jnp.bfloat16) * (DH ** (-0.5))).astype(jnp.bfloat16)
    kv_low = qkv[..., D:].astype(jnp.bfloat16)
    starts = []
    for step in range(experts // 2):
        row = (here // 2 + experts // 2 - step) % (experts // 2)
        starts += [(2 * row + here % 2) * rows, (2 * row + 1 - here % 2) * rows]
    metas, kv_pieces, att, lse = [], [], [], []
    for m in range(micro):
        metas.append(jnp.stack([lengths[m, 0], here * rows] + starts).astype(jnp.int32))
        kv_pieces.append(spread(kv_low[m], experts))
        out, norm = attend(metas[m], query[m], kv_pieces[m], near)
        att.append(out)
        lse.append(norm)
    attended = jnp.stack(att)
    x_mid = x_rows + matmul(attended.reshape(micro * rows, D), wout).reshape(micro, rows, D)
    h2 = rms_scale(x_mid, gains_f[:, 1]).astype(jnp.bfloat16)
    logits = matmul(h2, route_w)
    route_probs = jax.nn.softmax(logits, axis=-1)
    route_hot = (routes[..., None] == jnp.arange(experts, dtype=jnp.int32)).astype(jnp.float32)
    gates = jnp.sum(route_probs[:, :, None, :] * route_hot, axis=-1)
    positions = here * rows + jnp.arange(rows, dtype=jnp.int32)
    live = (positions[None, :] < lengths).astype(jnp.int32)
    slots = jax.vmap(lambda r, l: slot_tables(r, l, experts, capacity))(routes, live)
    columns = jnp.arange(experts * capacity, dtype=jnp.int32)
    hot = [(slots[:, :, j, None] == columns).astype(jnp.bfloat16) for j in range(TOP)]
    any_slot = hot[0] + hot[1]
    sent = jnp.einsum("mts,mtd->msd", any_slot, h2, preferred_element_type=jnp.float32)
    arrived = swap_slots(sent.astype(jnp.bfloat16), experts, capacity)
    joined = matmul(arrived, win)
    acted = geglu(joined).astype(jnp.bfloat16)
    produced = matmul(acted, wdown).astype(jnp.bfloat16)
    returned = swap_slots(produced, experts, capacity)
    picked = [
        jnp.einsum("mts,msd->mtd", hot[j], returned, preferred_element_type=jnp.float32)
        for j in range(TOP)
    ]
    grad_out = cotangent.astype(jnp.float32)
    block_out = x_mid + (gates[..., 0:1] * picked[0] + gates[..., 1:2] * picked[1])
    block_out = block_out.astype(jnp.bfloat16)
    grad_gates = jnp.stack([jnp.sum(grad_out * picked[j], axis=-1) for j in range(TOP)], axis=-1)
    grad_returned = sum(
        jnp.einsum(
            "mts,mtd->msd",
            hot[j],
            (gates[..., j : j + 1] * grad_out).astype(jnp.bfloat16),
            preferred_element_type=jnp.float32,
        )
        for j in range(TOP)
    ).astype(jnp.bfloat16)
    grad_produced = swap_slots(grad_returned, experts, capacity)
    sum_down = inner_rows(
        acted.reshape(-1, FF), grad_produced.reshape(-1, D)
    ).astype(jnp.bfloat16)
    out_down = lax.psum_scatter(sum_down[None], "dp", scatter_dimension=1, tiled=True)
    grad_acted = times_trans(grad_produced, wdown)
    grad_joined = jax.vjp(geglu, joined)[1](grad_acted)[0].astype(jnp.bfloat16)
    grad_arrived = times_trans(grad_joined, win).astype(jnp.bfloat16)
    grad_sent = swap_slots(grad_arrived, experts, capacity)
    sum_in = inner_rows(
        arrived.reshape(-1, D), grad_joined.reshape(-1, 2 * FF)
    ).astype(jnp.bfloat16)
    out_in = lax.psum_scatter(sum_in[None], "dp", scatter_dimension=1, tiled=True)
    grad_h2 = jnp.einsum("mts,msd->mtd", any_slot, grad_sent, preferred_element_type=jnp.float32)
    grad_route = jnp.sum(grad_gates[..., None] * route_hot, axis=2)
    grad_logits = route_probs * (
        grad_route - jnp.sum(route_probs * grad_route, axis=-1, keepdims=True)
    )
    grad_logits = grad_logits.astype(jnp.bfloat16)
    sum_router = inner_rows(h2.reshape(-1, D), grad_logits.reshape(-1, experts))
    grad_h2 = grad_h2 + times_trans(grad_logits, route_w)
    grad_mid, grad_gain_two = jax.vjp(rms_scale, x_mid, gains_f[:, 1])[1](grad_h2)
    grad_mid = grad_mid + grad_out
    grad_mid_low = grad_mid.astype(jnp.bfloat16)
    sum_out = inner_rows(attended.reshape(-1, D), grad_mid_low.reshape(-1, D))
    grad_attended = times_trans(grad_mid_low, wout).astype(jnp.bfloat16)
    grad_qkv, near_sum = [], 0.0
    for m in range(micro):
        outs = attend_back(
            metas[m], query[m], grad_attended[m], att[m], lse[m], kv_pieces[m], near
        )
        home = bring_home(outs[1:-1], experts).astype(jnp.bfloat16)
        near_sum = near_sum + outs[-1]
        grad_qkv.append(jnp.concatenate([outs[0], home[0], home[1]], axis=1))
    sum_bias = jnp.einsum(
        "hn,bn->bh",
        near_sum.reshape(H, -1),
        bucket_hot.astype(jnp.float32),
        precision=lax.Precision.HIGHEST,
    )
    grad_qkv = jnp.stack(grad_qkv)
    sum_qkv = inner_rows(h1.reshape(-1, D), grad_qkv.reshape(-1, 3 * D))
    grad_h1 = times_trans(grad_qkv, wqkv)
    grad_x, grad_gain_one = jax.vjp(rms_scale, x_rows, gains_f[:, 0])[1](grad_h1)
    grad_tokens = grad_x + grad_mid
    bias_rows = jnp.pad(
        sum_bias.reshape(D // own_rows, own_bias), ((0, 0), (0, own_rows - own_bias))
    ).reshape(D, 1)
    sums = jnp.concatenate(
        [
            sum_qkv,
            sum_out,
            grad_gain_one[:, None],
            grad_gain_two[:, None],
            sum_router,
            bias_rows,
            jnp.zeros((D, spare), jnp.float32),
        ],
        axis=1,
    ).astype(jnp.bfloat16)
    sums = lax.psum_scatter(sums, ("dp", "expert"), scatter_dimension=0, tiled=True)
    sums = sums.astype(jnp.float32)
    return (
        block_out,
        grad_tokens,
        sums[:, : 3 * D],
        sums[:, 3 * D : 4 * D],
        sums[:, 4 * D : 4 * D + 2],
        sums[:own_bias, 4 * D + 2 + experts],
        sums[:, 4 * D + 2 : 4 * D + 2 + experts],
        out_in.astype(jnp.float32),
        out_down.astype(jnp.float32),
    )


def solution(mesh):
    both = ("dp", "expert")
    in_specs = (
        P(None, both, None),
        P(None, "dp"),
        P(None, both, None),
        P(both, None),
        P(both, None),
        P(both, None),
        P(both),
        P(both, None),
        P("expert", "dp", None),
        P("expert", "dp", None),
        P(None, both, None),
    )
    out_specs = (
        P(None, both, None),
        P(None, both, None),
        P(both, None),
        P(both, None),
        P(both, None),
        P(both),
        P(both, None),
        P("expert", "dp", None),
        P("expert", "dp", None),
    )
    return jax.shard_map(local, mesh=mesh, in_specs=in_specs, out_specs=out_specs, check_vma=False)
```

```python
import jax
import jax.numpy as jnp
from jax import lax
from jax.experimental import pallas as pl
from jax.experimental.pallas import tpu as pltpu
from jax.sharding import PartitionSpec as P

D = 1024
H = 16
DH = 64
FF = 2816
BUCKETS = 32
TOP = 2
PAIRS = H // 2
LANES = 128

bucket_edges = (12, 16, 23, 32, 46, 64, 91)
norm_eps = 1e-06
MASKED = -1e30


def bucket_of(offset):
    dist = jnp.abs(offset)
    beyond = jnp.zeros_like(dist)
    for edge in bucket_edges:
        beyond = beyond + (dist >= edge).astype(jnp.int32)
    near = jnp.where(dist < 8, dist, 8 + beyond)
    return near + 16 * (offset > 0).astype(jnp.int32)


def rms_scale(values, gain):
    return values * lax.rsqrt(jnp.mean(values * values, axis=-1, keepdims=True) + norm_eps) * gain


def geglu(joined):
    half = joined.shape[-1] // 2
    return jax.nn.gelu(joined[..., :half], approximate=True) * joined[..., half:]


def slot_tables(route_rows, live, experts, capacity):
    count, top = route_rows.shape
    picks = (route_rows[:, :, None] == jnp.arange(experts, dtype=jnp.int32)[None, None, :]).astype(
        jnp.int32
    ) * live[:, None, None]
    flat = picks.reshape(count * top, experts)
    before = jnp.cumsum(flat, axis=0) - flat
    place = jnp.sum(before * flat, axis=1).reshape(count, top)
    kept = (place < capacity) & (live[:, None] > 0)
    return jnp.where(kept, route_rows * capacity + place, -1)


def matmul(left, right):
    return jnp.dot(left, right, preferred_element_type=jnp.float32)


def inner_rows(left, right):
    return jnp.einsum("...ti,...tj->ij", left, right, preferred_element_type=jnp.float32)


def times_trans(left, right):
    return jnp.einsum("...ti,ji->...tj", left, right, preferred_element_type=jnp.float32)


def lanes_dot(left, right):
    return lax.dot_general(
        left, right, (((1,), (1,)), ((), ())), preferred_element_type=jnp.float32
    )


def rows_dot(left, right):
    return lax.dot_general(
        left, right, (((0,), (0,)), ((), ())), preferred_element_type=jnp.float32
    )


def block_place(meta_ref, piece, part, blocks):
    place = meta_ref[2 + piece] // LANES + part - meta_ref[1] // LANES + 2
    return jnp.clip(place, 0, blocks - 1)


def attend_kernel(pieces, meta_ref, *refs):
    q_ref, kv_refs, near_ref = refs[0], refs[1 : 1 + 2 * pieces], refs[1 + 2 * pieces]
    att_ref, lse_ref, score_ref = refs[2 + 2 * pieces :]
    k_refs, v_refs = kv_refs[:pieces], kv_refs[pieces:]
    rows = q_ref.shape[0]
    blocks = near_ref.shape[1]
    length = meta_ref[0]
    query = q_ref[...]
    head_of = lax.broadcasted_iota(jnp.int32, (rows, LANES), 1) // DH
    row_head = lax.broadcasted_iota(jnp.int32, (LANES, rows), 0) // DH
    key_row = lax.broadcasted_iota(jnp.int32, (LANES, rows), 0)
    out = None
    for head in range(2):
        own = head_of == head
        query_own = jnp.where(own, query, jnp.zeros_like(query))
        top = jnp.full((1, rows), MASKED, jnp.float32)
        for piece in range(pieces):
            scores = lanes_dot(k_refs[piece][...], query_own)
            for part in range(rows // LANES):
                start = meta_ref[2 + piece] + part * LANES
                block = scores[part * LANES : (part + 1) * LANES]
                block = block + near_ref[head, block_place(meta_ref, piece, part, blocks)].astype(
                    jnp.float32
                )
                block = jnp.where(key_row < length - start, block, MASKED)
                score_ref[pl.ds(piece * rows + part * LANES, LANES), :] = block
                top = jnp.maximum(top, jnp.max(block, axis=0, keepdims=True))
        total = jnp.zeros((LANES, rows), jnp.float32)
        for piece in range(pieces):
            weights = jnp.exp(score_ref[pl.ds(piece * rows, rows), :] - top).astype(jnp.bfloat16)
            value = v_refs[piece][...]
            total = total + rows_dot(jnp.where(own, value, jnp.ones_like(value)), weights)
        other = (1 - head) * DH
        norm = total[other : other + 1]
        lse_ref[0, head : head + 1] = top + jnp.log(norm)
        scaled = total / norm
        out = scaled if out is None else jnp.where(row_head == 0, out, scaled)
    att_ref[...] = out.T.astype(jnp.bfloat16)


def attend_back_kernel(pieces, meta_ref, *refs):
    q_ref, grad_ref, att_ref, lse_ref = refs[:4]
    k_refs, v_refs = refs[4 : 4 + pieces], refs[4 + pieces : 4 + 2 * pieces]
    near_ref = refs[4 + 2 * pieces]
    dq_ref = refs[5 + 2 * pieces]
    dkv_refs = refs[6 + 2 * pieces : 6 + 3 * pieces]
    dnear_ref, block_ref = refs[6 + 3 * pieces :]
    rows = q_ref.shape[0]
    blocks = near_ref.shape[1]
    length = meta_ref[0]
    query = q_ref[...]
    grad = grad_ref[...]
    head_of = lax.broadcasted_iota(jnp.int32, (rows, LANES), 1) // DH
    row_head = lax.broadcasted_iota(jnp.int32, (LANES, rows), 0) // DH
    key_row = lax.broadcasted_iota(jnp.int32, (LANES, rows), 0)
    product = (grad.astype(jnp.float32) * att_ref[...].astype(jnp.float32)).T
    block_ref[...] = jnp.zeros_like(block_ref)
    zero = jnp.zeros_like(query)
    query_own = [jnp.where(head_of == head, query, zero) for head in range(2)]
    grad_own = [jnp.where(head_of == head, grad, zero) for head in range(2)]
    total = [jnp.zeros((LANES, rows), jnp.float32) for head in range(2)]
    delta = [jnp.sum(product[h * DH : (h + 1) * DH], axis=0, keepdims=True) for h in range(2)]
    for piece in range(pieces):
        keys = k_refs[piece][...]
        values = v_refs[piece][...]
        dk = jnp.zeros((rows, LANES), jnp.float32)
        dv = jnp.zeros((rows, LANES), jnp.float32)
        for head in range(2):
            scores = lanes_dot(keys, query_own[head])
            grad_probs = lanes_dot(values, grad_own[head])
            lse = lse_ref[0, head : head + 1]
            prob_parts, ds_parts = [], []
            for part in range(rows // LANES):
                start = meta_ref[2 + piece] + part * LANES
                place = block_place(meta_ref, piece, part, blocks)
                cut = slice(part * LANES, (part + 1) * LANES)
                block = scores[cut] + near_ref[head, place].astype(jnp.float32)
                block = jnp.where(key_row < length - start, block, MASKED)
                probs = jnp.exp(block - lse)
                ds = probs * (grad_probs[cut] - delta[head])
                block_ref[head, place] += ds
                prob_parts.append(probs.astype(jnp.bfloat16))
                ds_parts.append(ds.astype(jnp.bfloat16))
            probs_low = jnp.concatenate(prob_parts, axis=0)
            ds_low = jnp.concatenate(ds_parts, axis=0)
            dv = dv + matmul(probs_low, grad_own[head])
            dk = dk + matmul(ds_low, query_own[head])
            total[head] = total[head] + rows_dot(keys, ds_low)
        dkv_refs[piece][0] = dk.astype(jnp.bfloat16)
        dkv_refs[piece][1] = dv.astype(jnp.bfloat16)
    for head in range(2):
        for place in range(blocks):
            strips = jnp.zeros((8, rows + LANES), jnp.float32)
            for group in range(LANES // 8):
                strip = block_ref[head, place, group * 8 : (group + 1) * 8]
                strip = jnp.concatenate([strip, jnp.zeros((8, LANES), jnp.float32)], axis=1)
                strips = strips + pltpu.roll(strip, LANES - 8 - 8 * group, 1)
            dnear_ref[head, place] = strips
    out = jnp.where(row_head == 0, total[0], total[1])
    dq_ref[...] = (out.T * (DH ** (-0.5))).astype(jnp.bfloat16)


def attend(meta, query, kv_pieces, near):
    rows = query.shape[0]
    pieces = len(kv_pieces)
    blocks = near.shape[1]
    spec = pl.BlockSpec((rows, LANES), lambda i, m: (0, i))
    value_spec = pl.BlockSpec((rows, LANES), lambda i, m: (0, PAIRS + i))
    near_spec = pl.BlockSpec((2, blocks, LANES, rows), lambda i, m: (i, 0, 0, 0))
    lse_spec = pl.BlockSpec((1, 2, rows), lambda i, m: (i, 0, 0))
    flops = 4 * rows * rows * pieces * D
    return pl.pallas_call(
        lambda *refs: attend_kernel(pieces, *refs),
        out_shape=(
            jax.ShapeDtypeStruct((rows, D), jnp.bfloat16),
            jax.ShapeDtypeStruct((PAIRS, 2, rows), jnp.float32),
        ),
        grid_spec=pltpu.PrefetchScalarGridSpec(
            num_scalar_prefetch=1,
            grid=(PAIRS,),
            in_specs=[spec] + [spec] * pieces + [value_spec] * pieces + [near_spec],
            out_specs=[spec, lse_spec],
            scratch_shapes=[pltpu.VMEM((rows * pieces, rows), jnp.float32)],
        ),
        cost_estimate=pl.CostEstimate(
            flops=4 * flops, bytes_accessed=16 * 2**20, transcendentals=rows * rows * pieces * H
        ),
        name="attend",
    )(meta, query, *kv_pieces, *kv_pieces, near)


def attend_back(meta, query, grad, att, lse, kv_pieces, near):
    rows = query.shape[0]
    pieces = len(kv_pieces)
    blocks = near.shape[1]
    spec = pl.BlockSpec((rows, LANES), lambda i, m: (0, i))
    value_spec = pl.BlockSpec((rows, LANES), lambda i, m: (0, PAIRS + i))
    near_spec = pl.BlockSpec((2, blocks, LANES, rows), lambda i, m: (i, 0, 0, 0))
    lse_spec = pl.BlockSpec((1, 2, rows), lambda i, m: (i, 0, 0))
    dkv_spec = pl.BlockSpec((2, rows, LANES), lambda i, m: (0, 0, i))
    flops = 10 * rows * rows * pieces * D
    return pl.pallas_call(
        lambda *refs: attend_back_kernel(pieces, *refs),
        out_shape=(
            [jax.ShapeDtypeStruct((rows, D), jnp.bfloat16)]
            + [jax.ShapeDtypeStruct((2, rows, D), jnp.bfloat16)] * pieces
            + [jax.ShapeDtypeStruct((H, blocks, 8, rows + LANES), jnp.float32)]
        ),
        grid_spec=pltpu.PrefetchScalarGridSpec(
            num_scalar_prefetch=1,
            grid=(PAIRS,),
            in_specs=[spec, spec, spec, lse_spec]
            + [spec] * pieces
            + [value_spec] * pieces
            + [near_spec],
            out_specs=[spec]
            + [dkv_spec] * pieces
            + [pl.BlockSpec((2, blocks, 8, rows + LANES), lambda i, m: (i, 0, 0, 0))],
            scratch_shapes=[pltpu.VMEM((2, blocks, LANES, rows), jnp.float32)],
        ),
        cost_estimate=pl.CostEstimate(
            flops=4 * flops, bytes_accessed=32 * 2**20, transcendentals=rows * rows * pieces * H
        ),
        name="attend_back",
    )(meta, query, grad, att, lse, *kv_pieces, *kv_pieces, near)


def core_swap(values, experts):
    return lax.ppermute(values, "expert", [(e, e ^ 1) for e in range(experts)])


def row_shift(values, experts, step):
    return lax.ppermute(values, "expert", [(e, (e + 2 * step) % experts) for e in range(experts)])


def spread(values, experts):
    pieces = []
    for step in range(experts // 2):
        moved = row_shift(values, experts, step) if step else values
        pieces += [moved, core_swap(moved, experts)]
    return pieces


def bring_home(parts, experts):
    total = None
    for step in range(experts // 2):
        pair = parts[2 * step].astype(jnp.float32) + core_swap(parts[2 * step + 1], experts).astype(
            jnp.float32
        )
        if step:
            pair = row_shift(pair.astype(jnp.bfloat16), experts, -step).astype(jnp.float32)
        total = pair if total is None else total + pair
    return total


class Grid:
    def __init__(self):
        self.columns = lax.axis_size("expert") // 2
        self.rows = lax.axis_size("dp") // self.columns
        self.row = lax.axis_index("dp") // self.columns
        self.column = lax.axis_index("dp") % self.columns

    def shift(self, values, down, right):
        moves = []
        for z in range(self.rows):
            for x in range(self.columns):
                there = (z + down) % self.rows * self.columns + (x + right) % self.columns
                moves.append((z * self.columns + x, there))
        return lax.ppermute(values, "dp", moves)

    def place(self, z, x):
        return (z + self.rows) % self.rows * self.columns + (x + self.columns) % self.columns

    def ring(self, values, sideways):
        chain = [values]
        for _ in range((self.columns if sideways else self.rows) - 1):
            chain.append(self.shift(chain[-1], 0 if sideways else 1, 1 if sideways else 0))
        return chain

    def gather(self, values, buffer, at):
        for z, held in enumerate(self.ring(values, False)):
            for x, piece in enumerate(self.ring(held, True)):
                start = (self.place(self.row - z, self.column - x), at) + (0,) * (values.ndim - 1)
                buffer = lax.dynamic_update_slice(buffer, piece[None], start)
        return buffer

    def gather_sideways_first(self, values, buffer, at):
        strip = jnp.stack(self.ring(values, True))
        for z, held in enumerate(self.ring(strip, False)):
            for x in range(self.columns):
                start = (self.place(self.row - z, self.column - x), at) + (0,) * (values.ndim - 1)
                buffer = lax.dynamic_update_slice(buffer, held[x][None], start)
        return buffer

    def reduce(self, parts):
        def term(z, x):
            return lax.dynamic_index_in_dim(parts, self.place(z, x), 0, False)

        run = None
        for down in range(self.rows):
            z = self.row - 1 - down
            line = term(z, self.column - 1)
            for right in range(1, self.columns):
                line = add_low(self.shift(line, 0, 1), term(z, self.column - 1 - right))
            run = line if run is None else add_low(self.shift(run, 1, 0), line)
        return run

    def reduce_down_first(self, parts):
        grid = parts.reshape((self.rows, self.columns) + parts.shape[1:])
        run = None
        for down in range(self.rows):
            z = (self.row - 1 - down + self.rows) % self.rows
            line = lax.dynamic_index_in_dim(grid, z, 0, False)
            run = line if run is None else add_low(self.shift(run, 1, 0), line)

        def term(x):
            return lax.dynamic_index_in_dim(run, (x + self.columns) % self.columns, 0, False)

        line = term(self.column - 1)
        for right in range(1, self.columns):
            line = add_low(self.shift(line, 0, 1), term(self.column - 1 - right))
        return line


def add_low(left, right):
    return (left.astype(jnp.float32) + right.astype(jnp.float32)).astype(jnp.bfloat16)


def swap_slots(values, experts, capacity):
    micro = values.shape[0]
    moved = lax.all_to_all(
        values.reshape(micro, experts, capacity, D),
        "expert",
        split_axis=1,
        concat_axis=1,
        tiled=True,
    )
    return moved.reshape(micro, experts * capacity, D)


def local(
    tokens, lengths, routes, w_qkv, w_out, norm_gains, bias_table, router, w_in, w_down, cotangent
):
    micro, rows, width = tokens.shape
    experts = lax.axis_size("expert")
    here = lax.axis_index("expert")
    capacity = (5 * rows * TOP + 4 * experts - 1) // (4 * experts)
    own_rows = w_qkv.shape[0]
    own_bias = bias_table.shape[0]
    spare = LANES - 3 - experts

    packed = jnp.concatenate(
        [
            w_qkv,
            w_out,
            norm_gains,
            router,
            jnp.pad(bias_table, (0, own_rows - own_bias))[:, None],
            jnp.zeros((own_rows, spare), jnp.bfloat16),
        ],
        axis=1,
    )
    packed = lax.all_gather(packed, ("dp", "expert"), axis=0, tiled=True)
    wqkv = packed[:, : 3 * D]
    wout = packed[:, 3 * D : 4 * D]
    misc = packed[:, 4 * D :]
    gains_f = misc[:, :2].astype(jnp.float32)
    route_w = misc[:, 2 : 2 + experts]
    table = misc[:, 2 + experts].reshape(D // own_rows, own_rows)[:, :own_bias]
    table = table.reshape(BUCKETS, H)
    grid = Grid()
    many = grid.rows * grid.columns
    half = w_down.shape[1] // 2
    win = grid.gather(w_in[0], jnp.zeros((many,) + w_in.shape[1:], jnp.bfloat16), 0)
    win = win.reshape(D, 2 * FF)
    wdown = jnp.zeros((many,) + w_down.shape[1:], jnp.bfloat16)
    wdown = grid.gather_sideways_first(w_down[0, half:], wdown, half)
    wdown = grid.gather(w_down[0, :half], wdown, 0).reshape(FF, D)

    blocks = rows // LANES + 4
    block_at = jnp.arange(blocks, dtype=jnp.int32)[:, None, None] - 2
    key_at = jnp.arange(LANES, dtype=jnp.int32)[None, :, None]
    query_at = jnp.arange(rows, dtype=jnp.int32)[None, None, :]
    bucket = bucket_of(block_at * LANES + key_at - query_at).reshape(-1)
    bucket_hot = (bucket[None, :] == jnp.arange(BUCKETS, dtype=jnp.int32)[:, None]).astype(
        jnp.bfloat16
    )
    near = jnp.einsum("bh,bn->hn", table, bucket_hot, preferred_element_type=jnp.float32)
    near = near.astype(jnp.bfloat16).reshape(H, blocks, LANES, rows)

    x_rows = tokens.astype(jnp.float32)
    h1 = rms_scale(x_rows, gains_f[:, 0]).astype(jnp.bfloat16)
    qkv = matmul(h1.reshape(micro * rows, D), wqkv)
    qkv = qkv.reshape(micro, rows, 3 * D)
    query = (qkv[..., :D].astype(jnp.bfloat16) * (DH ** (-0.5))).astype(jnp.bfloat16)
    kv_low = qkv[..., D:].astype(jnp.bfloat16)
    starts = []
    for step in range(experts // 2):
        row = (here // 2 + experts // 2 - step) % (experts // 2)
        starts += [(2 * row + here % 2) * rows, (2 * row + 1 - here % 2) * rows]
    metas, kv_pieces, att, lse = [], [], [], []
    for m in range(micro):
        metas.append(jnp.stack([lengths[m, 0], here * rows] + starts).astype(jnp.int32))
        kv_pieces.append(spread(kv_low[m], experts))
        out, norm = attend(metas[m], query[m], kv_pieces[m], near)
        att.append(out)
        lse.append(norm)
    attended = jnp.stack(att)
    x_mid = x_rows + matmul(attended.reshape(micro * rows, D), wout).reshape(micro, rows, D)
    h2 = rms_scale(x_mid, gains_f[:, 1]).astype(jnp.bfloat16)
    logits = matmul(h2, route_w)
    route_probs = jax.nn.softmax(logits, axis=-1)
    route_hot = (routes[..., None] == jnp.arange(experts, dtype=jnp.int32)).astype(jnp.float32)
    gates = jnp.sum(route_probs[:, :, None, :] * route_hot, axis=-1)
    positions = here * rows + jnp.arange(rows, dtype=jnp.int32)
    live = (positions[None, :] < lengths).astype(jnp.int32)
    slots = jax.vmap(lambda r, l: slot_tables(r, l, experts, capacity))(routes, live)
    columns = jnp.arange(experts * capacity, dtype=jnp.int32)
    hot = [(slots[:, :, j, None] == columns).astype(jnp.bfloat16) for j in range(TOP)]
    any_slot = hot[0] + hot[1]
    sent = jnp.einsum("mts,mtd->msd", any_slot, h2, preferred_element_type=jnp.float32)
    grad_out = cotangent.astype(jnp.float32)
    grad_returned = sum(
        jnp.einsum(
            "mts,mtd->msd",
            hot[j],
            (gates[..., j : j + 1] * grad_out).astype(jnp.bfloat16),
            preferred_element_type=jnp.float32,
        )
        for j in range(TOP)
    )
    both = jnp.concatenate([sent, grad_returned], axis=0).astype(jnp.bfloat16)
    both = swap_slots(both, experts, capacity)
    arrived, grad_produced = both[:micro], both[micro:]
    joined = matmul(arrived, win)
    acted = geglu(joined).astype(jnp.bfloat16)
    produced = matmul(acted, wdown).astype(jnp.bfloat16)
    returned = swap_slots(produced, experts, capacity)
    picked = [
        jnp.einsum("mts,msd->mtd", hot[j], returned, preferred_element_type=jnp.float32)
        for j in range(TOP)
    ]
    block_out = x_mid + (gates[..., 0:1] * picked[0] + gates[..., 1:2] * picked[1])
    block_out = block_out.astype(jnp.bfloat16)
    grad_gates = jnp.stack([jnp.sum(grad_out * picked[j], axis=-1) for j in range(TOP)], axis=-1)
    sum_down = inner_rows(
        acted.reshape(-1, FF), grad_produced.reshape(-1, D)
    ).astype(jnp.bfloat16)
    sum_down = sum_down.reshape(many, FF // many, D)
    out_down = jnp.concatenate(
        [grid.reduce(sum_down[:, :half]), grid.reduce_down_first(sum_down[:, half:])], axis=0
    )[None]
    grad_acted = times_trans(grad_produced, wdown)
    grad_joined = jax.vjp(geglu, joined)[1](grad_acted)[0].astype(jnp.bfloat16)
    grad_sent = jnp.concatenate(
        [
            swap_slots(
                times_trans(grad_joined[m : m + 1], win).astype(jnp.bfloat16), experts, capacity
            )
            for m in range(micro)
        ],
        axis=0,
    )
    sum_in = inner_rows(
        arrived.reshape(-1, D), grad_joined.reshape(-1, 2 * FF)
    ).astype(jnp.bfloat16)
    out_in = grid.reduce(sum_in.reshape(many, D // many, 2 * FF))[None]
    grad_h2 = jnp.einsum("mts,msd->mtd", any_slot, grad_sent, preferred_element_type=jnp.float32)
    grad_route = jnp.sum(grad_gates[..., None] * route_hot, axis=2)
    grad_logits = route_probs * (
        grad_route - jnp.sum(route_probs * grad_route, axis=-1, keepdims=True)
    )
    grad_logits = grad_logits.astype(jnp.bfloat16)
    sum_router = inner_rows(h2.reshape(-1, D), grad_logits.reshape(-1, experts))
    grad_h2 = grad_h2 + times_trans(grad_logits, route_w)
    grad_mid, grad_gain_two = jax.vjp(rms_scale, x_mid, gains_f[:, 1])[1](grad_h2)
    grad_mid = grad_mid + grad_out
    grad_mid_low = grad_mid.astype(jnp.bfloat16)
    sum_out = inner_rows(attended.reshape(-1, D), grad_mid_low.reshape(-1, D))
    grad_attended = times_trans(grad_mid_low, wout).astype(jnp.bfloat16)
    grad_qkv, near_sum = [], 0.0
    for m in range(micro):
        outs = attend_back(
            metas[m], query[m], grad_attended[m], att[m], lse[m], kv_pieces[m], near
        )
        home = bring_home(outs[1:-1], experts).astype(jnp.bfloat16)
        near_sum = near_sum + outs[-1]
        grad_qkv.append(jnp.concatenate([outs[0], home[0], home[1]], axis=1))
    strip_at = jnp.arange(8, dtype=jnp.int32)[None, :, None] + LANES - 8
    column_at = jnp.arange(rows + LANES, dtype=jnp.int32)[None, None, :]
    strip_bucket = bucket_of(block_at * LANES + strip_at - column_at).reshape(-1)
    strip_hot = (strip_bucket[None, :] == jnp.arange(BUCKETS, dtype=jnp.int32)[:, None]).astype(
        jnp.float32
    )
    sum_bias = jnp.einsum(
        "hn,bn->bh", near_sum.reshape(H, -1), strip_hot, precision=lax.Precision.HIGHEST
    )
    grad_qkv = jnp.stack(grad_qkv)
    sum_qkv = inner_rows(h1.reshape(-1, D), grad_qkv.reshape(-1, 3 * D))
    grad_h1 = times_trans(grad_qkv, wqkv)
    grad_x, grad_gain_one = jax.vjp(rms_scale, x_rows, gains_f[:, 0])[1](grad_h1)
    grad_tokens = grad_x + grad_mid
    bias_rows = jnp.pad(
        sum_bias.reshape(D // own_rows, own_bias), ((0, 0), (0, own_rows - own_bias))
    ).reshape(D, 1)
    sums = jnp.concatenate(
        [
            sum_qkv,
            sum_out,
            grad_gain_one[:, None],
            grad_gain_two[:, None],
            sum_router,
            bias_rows,
            jnp.zeros((D, spare), jnp.float32),
        ],
        axis=1,
    ).astype(jnp.bfloat16)
    sums = lax.psum_scatter(sums, ("dp", "expert"), scatter_dimension=0, tiled=True)
    sums = sums.astype(jnp.float32)
    return (
        block_out,
        grad_tokens,
        sums[:, : 3 * D],
        sums[:, 3 * D : 4 * D],
        sums[:, 4 * D : 4 * D + 2],
        sums[:own_bias, 4 * D + 2 + experts],
        sums[:, 4 * D + 2 : 4 * D + 2 + experts],
        out_in.astype(jnp.float32),
        out_down.astype(jnp.float32),
    )


def solution(mesh):
    both = ("dp", "expert")
    in_specs = (
        P(None, both, None),
        P(None, "dp"),
        P(None, both, None),
        P(both, None),
        P(both, None),
        P(both, None),
        P(both),
        P(both, None),
        P("expert", "dp", None),
        P("expert", "dp", None),
        P(None, both, None),
    )
    out_specs = (
        P(None, both, None),
        P(None, both, None),
        P(both, None),
        P(both, None),
        P(both, None),
        P(both),
        P(both, None),
        P("expert", "dp", None),
        P("expert", "dp", None),
    )
    return jax.shard_map(local, mesh=mesh, in_specs=in_specs, out_specs=out_specs, check_vma=False)
```

```python
import jax
import jax.numpy as jnp
from jax import lax
from jax.experimental import pallas as pl
from jax.experimental.pallas import tpu as pltpu
from jax.sharding import PartitionSpec as P

D = 1024
H = 16
DH = 64
FF = 2816
BUCKETS = 32
TOP = 2
PAIRS = H // 2
LANES = 128

bucket_edges = (12, 16, 23, 32, 46, 64, 91)
norm_eps = 1e-06
MASKED = -1e30


def bucket_of(offset):
    dist = jnp.abs(offset)
    beyond = jnp.zeros_like(dist)
    for edge in bucket_edges:
        beyond = beyond + (dist >= edge).astype(jnp.int32)
    near = jnp.where(dist < 8, dist, 8 + beyond)
    return near + 16 * (offset > 0).astype(jnp.int32)


def rms_scale(values, gain):
    return values * lax.rsqrt(jnp.mean(values * values, axis=-1, keepdims=True) + norm_eps) * gain


def geglu(joined):
    half = joined.shape[-1] // 2
    return jax.nn.gelu(joined[..., :half], approximate=True) * joined[..., half:]


def slot_tables(route_rows, live, experts, capacity):
    count, top = route_rows.shape
    picks = (route_rows[:, :, None] == jnp.arange(experts, dtype=jnp.int32)[None, None, :]).astype(
        jnp.int32
    ) * live[:, None, None]
    flat = picks.reshape(count * top, experts)
    before = jnp.cumsum(flat, axis=0) - flat
    place = jnp.sum(before * flat, axis=1).reshape(count, top)
    kept = (place < capacity) & (live[:, None] > 0)
    return jnp.where(kept, route_rows * capacity + place, -1)


def matmul(left, right):
    return jnp.dot(left, right, preferred_element_type=jnp.float32)


def inner_rows(left, right):
    return jnp.einsum("...ti,...tj->ij", left, right, preferred_element_type=jnp.float32)


def times_trans(left, right):
    return jnp.einsum("...ti,ji->...tj", left, right, preferred_element_type=jnp.float32)


def lanes_dot(left, right):
    return lax.dot_general(
        left, right, (((1,), (1,)), ((), ())), preferred_element_type=jnp.float32
    )


def rows_dot(left, right):
    return lax.dot_general(
        left, right, (((0,), (0,)), ((), ())), preferred_element_type=jnp.float32
    )


def block_place(meta_ref, piece, part, blocks):
    place = meta_ref[2 + piece] // LANES + part - meta_ref[1] // LANES + 2
    return jnp.clip(place, 0, blocks - 1)


def attend_kernel(pieces, meta_ref, *refs):
    q_ref, kv_refs, near_ref = refs[0], refs[1 : 1 + 2 * pieces], refs[1 + 2 * pieces]
    att_ref, lse_ref, score_ref = refs[2 + 2 * pieces :]
    k_refs, v_refs = kv_refs[:pieces], kv_refs[pieces:]
    rows = q_ref.shape[0]
    blocks = near_ref.shape[1]
    length = meta_ref[0]
    query = q_ref[...]
    head_of = lax.broadcasted_iota(jnp.int32, (rows, LANES), 1) // DH
    row_head = lax.broadcasted_iota(jnp.int32, (LANES, rows), 0) // DH
    key_row = lax.broadcasted_iota(jnp.int32, (LANES, rows), 0)
    out = None
    for head in range(2):
        own = head_of == head
        query_own = jnp.where(own, query, jnp.zeros_like(query))
        top = jnp.full((1, rows), MASKED, jnp.float32)
        for piece in range(pieces):
            scores = lanes_dot(k_refs[piece][...], query_own)
            for part in range(rows // LANES):
                start = meta_ref[2 + piece] + part * LANES
                block = scores[part * LANES : (part + 1) * LANES]
                block = block + near_ref[head, block_place(meta_ref, piece, part, blocks)].astype(
                    jnp.float32
                )
                block = jnp.where(key_row < length - start, block, MASKED)
                score_ref[pl.ds(piece * rows + part * LANES, LANES), :] = block
                top = jnp.maximum(top, jnp.max(block, axis=0, keepdims=True))
        total = jnp.zeros((LANES, rows), jnp.float32)
        for piece in range(pieces):
            weights = jnp.exp(score_ref[pl.ds(piece * rows, rows), :] - top).astype(jnp.bfloat16)
            value = v_refs[piece][...]
            total = total + rows_dot(jnp.where(own, value, jnp.ones_like(value)), weights)
        other = (1 - head) * DH
        norm = total[other : other + 1]
        lse_ref[0, head : head + 1] = top + jnp.log(norm)
        scaled = total / norm
        out = scaled if out is None else jnp.where(row_head == 0, out, scaled)
    att_ref[...] = out.T.astype(jnp.bfloat16)


def attend_back_kernel(pieces, meta_ref, *refs):
    q_ref, grad_ref, att_ref, lse_ref = refs[:4]
    k_refs, v_refs = refs[4 : 4 + pieces], refs[4 + pieces : 4 + 2 * pieces]
    near_ref = refs[4 + 2 * pieces]
    dq_ref = refs[5 + 2 * pieces]
    dkv_refs = refs[6 + 2 * pieces : 6 + 3 * pieces]
    dnear_ref, block_ref = refs[6 + 3 * pieces :]
    rows = q_ref.shape[0]
    blocks = near_ref.shape[1]
    length = meta_ref[0]
    query = q_ref[...]
    grad = grad_ref[...]
    head_of = lax.broadcasted_iota(jnp.int32, (rows, LANES), 1) // DH
    row_head = lax.broadcasted_iota(jnp.int32, (LANES, rows), 0) // DH
    key_row = lax.broadcasted_iota(jnp.int32, (LANES, rows), 0)
    product = (grad.astype(jnp.float32) * att_ref[...].astype(jnp.float32)).T
    block_ref[...] = jnp.zeros_like(block_ref)
    zero = jnp.zeros_like(query)
    query_own = [jnp.where(head_of == head, query, zero) for head in range(2)]
    grad_own = [jnp.where(head_of == head, grad, zero) for head in range(2)]
    total = [jnp.zeros((LANES, rows), jnp.float32) for head in range(2)]
    delta = [jnp.sum(product[h * DH : (h + 1) * DH], axis=0, keepdims=True) for h in range(2)]
    for piece in range(pieces):
        keys = k_refs[piece][...]
        values = v_refs[piece][...]
        dk = jnp.zeros((rows, LANES), jnp.float32)
        dv = jnp.zeros((rows, LANES), jnp.float32)
        for head in range(2):
            scores = lanes_dot(keys, query_own[head])
            grad_probs = lanes_dot(values, grad_own[head])
            lse = lse_ref[0, head : head + 1]
            prob_parts, ds_parts = [], []
            for part in range(rows // LANES):
                start = meta_ref[2 + piece] + part * LANES
                place = block_place(meta_ref, piece, part, blocks)
                cut = slice(part * LANES, (part + 1) * LANES)
                block = scores[cut] + near_ref[head, place].astype(jnp.float32)
                block = jnp.where(key_row < length - start, block, MASKED)
                probs = jnp.exp(block - lse)
                ds = probs * (grad_probs[cut] - delta[head])
                block_ref[head, place] += ds
                prob_parts.append(probs.astype(jnp.bfloat16))
                ds_parts.append(ds.astype(jnp.bfloat16))
            probs_low = jnp.concatenate(prob_parts, axis=0)
            ds_low = jnp.concatenate(ds_parts, axis=0)
            dv = dv + matmul(probs_low, grad_own[head])
            dk = dk + matmul(ds_low, query_own[head])
            total[head] = total[head] + rows_dot(keys, ds_low)
        dkv_refs[piece][0] = dk.astype(jnp.bfloat16)
        dkv_refs[piece][1] = dv.astype(jnp.bfloat16)
    for head in range(2):
        for place in range(blocks):
            strips = jnp.zeros((8, rows + LANES), jnp.float32)
            for group in range(LANES // 8):
                strip = block_ref[head, place, group * 8 : (group + 1) * 8]
                strip = jnp.concatenate([strip, jnp.zeros((8, LANES), jnp.float32)], axis=1)
                strips = strips + pltpu.roll(strip, LANES - 8 - 8 * group, 1)
            dnear_ref[head, place] = strips
    out = jnp.where(row_head == 0, total[0], total[1])
    dq_ref[...] = (out.T * (DH ** (-0.5))).astype(jnp.bfloat16)


def attend(meta, query, kv_pieces, near):
    rows = query.shape[0]
    pieces = len(kv_pieces)
    blocks = near.shape[1]
    spec = pl.BlockSpec((rows, LANES), lambda i, m: (0, i))
    value_spec = pl.BlockSpec((rows, LANES), lambda i, m: (0, PAIRS + i))
    near_spec = pl.BlockSpec((2, blocks, LANES, rows), lambda i, m: (i, 0, 0, 0))
    lse_spec = pl.BlockSpec((1, 2, rows), lambda i, m: (i, 0, 0))
    flops = 4 * rows * rows * pieces * D
    return pl.pallas_call(
        lambda *refs: attend_kernel(pieces, *refs),
        out_shape=(
            jax.ShapeDtypeStruct((rows, D), jnp.bfloat16),
            jax.ShapeDtypeStruct((PAIRS, 2, rows), jnp.float32),
        ),
        grid_spec=pltpu.PrefetchScalarGridSpec(
            num_scalar_prefetch=1,
            grid=(PAIRS,),
            in_specs=[spec] + [spec] * pieces + [value_spec] * pieces + [near_spec],
            out_specs=[spec, lse_spec],
            scratch_shapes=[pltpu.VMEM((rows * pieces, rows), jnp.float32)],
        ),
        cost_estimate=pl.CostEstimate(
            flops=4 * flops, bytes_accessed=16 * 2**20, transcendentals=rows * rows * pieces * H
        ),
        name="attend",
    )(meta, query, *kv_pieces, *kv_pieces, near)


def attend_back(meta, query, grad, att, lse, kv_pieces, near):
    rows = query.shape[0]
    pieces = len(kv_pieces)
    blocks = near.shape[1]
    spec = pl.BlockSpec((rows, LANES), lambda i, m: (0, i))
    value_spec = pl.BlockSpec((rows, LANES), lambda i, m: (0, PAIRS + i))
    near_spec = pl.BlockSpec((2, blocks, LANES, rows), lambda i, m: (i, 0, 0, 0))
    lse_spec = pl.BlockSpec((1, 2, rows), lambda i, m: (i, 0, 0))
    dkv_spec = pl.BlockSpec((2, rows, LANES), lambda i, m: (0, 0, i))
    flops = 10 * rows * rows * pieces * D
    return pl.pallas_call(
        lambda *refs: attend_back_kernel(pieces, *refs),
        out_shape=(
            [jax.ShapeDtypeStruct((rows, D), jnp.bfloat16)]
            + [jax.ShapeDtypeStruct((2, rows, D), jnp.bfloat16)] * pieces
            + [jax.ShapeDtypeStruct((H, blocks, 8, rows + LANES), jnp.float32)]
        ),
        grid_spec=pltpu.PrefetchScalarGridSpec(
            num_scalar_prefetch=1,
            grid=(PAIRS,),
            in_specs=[spec, spec, spec, lse_spec]
            + [spec] * pieces
            + [value_spec] * pieces
            + [near_spec],
            out_specs=[spec]
            + [dkv_spec] * pieces
            + [pl.BlockSpec((2, blocks, 8, rows + LANES), lambda i, m: (i, 0, 0, 0))],
            scratch_shapes=[pltpu.VMEM((2, blocks, LANES, rows), jnp.float32)],
        ),
        cost_estimate=pl.CostEstimate(
            flops=4 * flops, bytes_accessed=32 * 2**20, transcendentals=rows * rows * pieces * H
        ),
        name="attend_back",
    )(meta, query, grad, att, lse, *kv_pieces, *kv_pieces, near)


def core_swap(values, experts):
    return lax.ppermute(values, "expert", [(e, e ^ 1) for e in range(experts)])


def row_shift(values, experts, step):
    return lax.ppermute(values, "expert", [(e, (e + 2 * step) % experts) for e in range(experts)])


def spread(values, experts):
    pieces = []
    for step in range(experts // 2):
        moved = row_shift(values, experts, step) if step else values
        pieces += [moved, core_swap(moved, experts)]
    return pieces


def bring_home(parts, experts):
    total = None
    for step in range(experts // 2):
        pair = parts[2 * step].astype(jnp.float32) + core_swap(parts[2 * step + 1], experts).astype(
            jnp.float32
        )
        if step:
            pair = row_shift(pair.astype(jnp.bfloat16), experts, -step).astype(jnp.float32)
        total = pair if total is None else total + pair
    return total


class Grid:
    def __init__(self):
        self.columns = lax.axis_size("expert") // 2
        self.rows = lax.axis_size("dp") // self.columns
        self.row = lax.axis_index("dp") // self.columns
        self.column = lax.axis_index("dp") % self.columns

    def shift(self, values, down, right):
        moves = []
        for z in range(self.rows):
            for x in range(self.columns):
                there = (z + down) % self.rows * self.columns + (x + right) % self.columns
                moves.append((z * self.columns + x, there))
        return lax.ppermute(values, "dp", moves)

    def place(self, z, x):
        return (z + self.rows) % self.rows * self.columns + (x + self.columns) % self.columns

    def ring(self, values, sideways):
        chain = [values]
        for _ in range((self.columns if sideways else self.rows) - 1):
            chain.append(self.shift(chain[-1], 0 if sideways else 1, 1 if sideways else 0))
        return chain


def tie(values, transfers):
    return lax.optimization_barrier((values, transfers))


class WeightGather:
    def __init__(self, grid, w_in, w_down):
        many = grid.rows * grid.columns
        self.grid = grid
        self.half = w_down.shape[0] // 2
        self.step = 0
        self.held = [w_in, w_down[: self.half]]
        self.strip = w_down[self.half :]
        self.win = jnp.zeros((many,) + w_in.shape, jnp.bfloat16)
        self.wdown = jnp.zeros((many,) + w_down.shape, jnp.bfloat16)

    def start(self):
        grid = self.grid
        last = self.step == grid.rows - 1
        down = None if last else [grid.shift(h, 1, 0) for h in self.held]
        side = [grid.ring(h, True)[1:] for h in self.held]
        if self.step == 0:
            strip = grid.ring(self.strip, True)[1:]
        else:
            strip = grid.shift(self.strip, 1, 0)
        self.moving = (down, side, strip)

    def put(self, x, piece_in, piece_down, half_down, at):
        grid = self.grid
        there = grid.place(grid.row - self.step, grid.column - x)
        if piece_in is not None:
            self.win = lax.dynamic_update_slice(self.win, piece_in[None], (there, 0, 0))
            self.wdown = lax.dynamic_update_slice(self.wdown, piece_down[None], (there, 0, 0))
        if half_down is not None:
            self.wdown = lax.dynamic_update_slice(self.wdown, half_down[None], (there, at, 0))

    def finish(self, values):
        grid = self.grid
        values, (down, side, strip) = tie(values, self.moving)
        if self.step == 0:
            self.strip = jnp.stack([self.strip] + strip)
        else:
            self.strip = strip
        for x in range(grid.columns):
            pieces = self.held if x == 0 else [s[x - 1] for s in side]
            self.put(x, pieces[0], pieces[1], self.strip[x], self.half)
        self.held = down
        self.step += 1
        if self.step < grid.rows:
            self.start()
        return values

    def result(self, values):
        while self.step < self.grid.rows:
            values = self.finish(values)
        return values, self.win.reshape(D, 2 * FF), self.wdown.reshape(FF, D)


class WeightReduce:
    def __init__(self, grid, sum_in, sum_down):
        many = grid.rows * grid.columns
        self.grid = grid
        self.half = FF // many // 2
        self.step = 0
        down = sum_down.reshape(many, FF // many, D)
        self.parts = [sum_in.reshape(many, D // many, 2 * FF), down[:, : self.half]]
        self.strips = down[:, self.half :].reshape(grid.rows, grid.columns, self.half, D)
        self.run = None
        self.strip = self.strip_term(0)
        self.start()

    def term(self, part, x):
        there = self.grid.place(self.grid.row - 1 - self.step, x)
        return lax.dynamic_index_in_dim(part, there, 0, False)

    def strip_term(self, step):
        z = (self.grid.row - 1 - step + self.grid.rows) % self.grid.rows
        return lax.dynamic_index_in_dim(self.strips, z, 0, False)

    def sideways(self, term):
        grid = self.grid
        line = term(grid.column - 1)
        for right in range(1, grid.columns):
            moved = grid.shift(line, 0, 1)
            if right == grid.columns - 1:
                return moved
            line = add_low(moved, term(grid.column - 1 - right))

    def start(self):
        grid = self.grid
        side = [self.sideways(lambda x, p=p: self.term(p, x)) for p in self.parts]
        down = None if self.run is None else [grid.shift(r, 1, 0) for r in self.run]
        if self.step < grid.rows - 1:
            strip = grid.shift(self.strip, 1, 0)
        else:
            strip = self.sideways(self.strip_at)
        self.moving = (side, down, strip)

    def strip_at(self, x):
        x = (x + self.grid.columns) % self.grid.columns
        return lax.dynamic_index_in_dim(self.strip, x, 0, False)

    def finish(self, values):
        grid = self.grid
        values, (self.moving, self.parts) = tie(values, (self.moving, self.parts))
        side, down, strip = self.moving
        lines = []
        for index, part in enumerate(self.parts):
            own = self.term(part, grid.column)
            total = side[index].astype(jnp.float32) + own.astype(jnp.float32)
            if down is not None:
                total = total + down[index].astype(jnp.float32)
            lines.append(total.astype(jnp.bfloat16))
        self.run = lines
        if self.step < grid.rows - 1:
            self.strip = add_low(strip, self.strip_term(self.step + 1))
        else:
            self.strip = add_low(strip, self.strip_at(grid.column))
        self.step += 1
        if self.step < grid.rows:
            self.start()
        return values

    def result(self, values):
        while self.step < self.grid.rows:
            values = self.finish(values)
        return values, self.run[0], jnp.concatenate([self.run[1], self.strip], axis=0)


def add_low(left, right):
    return (left.astype(jnp.float32) + right.astype(jnp.float32)).astype(jnp.bfloat16)


class Flow:
    def __init__(self, steps):
        self.steps = steps
        self.result = None
        self.step(None)

    def step(self, landed):
        try:
            self.moving = self.steps.send(landed)
        except StopIteration as end:
            self.result, self.steps, self.moving = end.value, None, None


def advance(values, *flows):
    flows = [flow for flow in flows if flow.steps is not None]
    values, landed = tie(values, [flow.moving for flow in flows])
    for flow, moved in zip(flows, landed):
        flow.step(moved)
    return values


def ring_sum(parts, axis, place, count, shift):
    def term(step):
        return lax.dynamic_index_in_dim(
            parts, (place - 1 - step + 2 * count) % count, axis, False
        )

    run = term(0)
    for step in range(1, count):
        run = add_low((yield shift(run)), term(step))
    return run


def side_by_side(left, right):
    flows = [Flow(left), Flow(right)]
    while any(flow.steps is not None for flow in flows):
        landed = yield [flow.moving for flow in flows]
        for flow, moved in zip(flows, landed):
            if flow.steps is not None:
                flow.step(moved)
    return [flow.result for flow in flows]


def scatter_sum(values, grid, experts):
    lines = experts // 2
    here = lax.axis_index("expert")
    columns = values.shape[1]
    own = values.shape[0] // (grid.rows * grid.columns * experts)
    parts = values.reshape(grid.rows, grid.columns, lines, 2, own, columns)
    parts = yield from ring_sum(parts, 3, here % 2, 2, lambda v: core_swap(v, experts))
    cut = columns // (2 * LANES) * LANES

    def over_y(v, axis):
        return ring_sum(v, axis, here // 2, lines, lambda u: row_shift(u, experts, 1))

    def over_x(v, axis):
        return ring_sum(v, axis, grid.column, grid.columns, lambda u: grid.shift(u, 0, 1))

    def over_z(v):
        return ring_sum(v, 0, grid.row, grid.rows, lambda u: grid.shift(u, 1, 0))

    def left():
        v = yield from over_y(parts[..., :cut], 2)
        v = yield from over_x(v, 1)
        return (yield from over_z(v))

    def right():
        v = yield from over_x(parts[..., cut:], 1)
        v = yield from over_y(v, 1)
        return (yield from over_z(v))

    halves = yield from side_by_side(left(), right())
    return jnp.concatenate(halves, axis=1).astype(jnp.float32)


def swap_slots(values, experts, capacity):
    micro = values.shape[0]
    moved = lax.all_to_all(
        values.reshape(micro, experts, capacity, D),
        "expert",
        split_axis=1,
        concat_axis=1,
        tiled=True,
    )
    return moved.reshape(micro, experts * capacity, D)


def local(
    tokens, lengths, routes, w_qkv, w_out, norm_gains, bias_table, router, w_in, w_down, cotangent
):
    micro, rows, width = tokens.shape
    experts = lax.axis_size("expert")
    here = lax.axis_index("expert")
    capacity = (5 * rows * TOP + 4 * experts - 1) // (4 * experts)
    own_rows = w_qkv.shape[0]
    own_bias = bias_table.shape[0]
    spare = LANES - 3 - experts

    grid = Grid()

    packed = jnp.concatenate(
        [
            w_qkv,
            w_out,
            norm_gains,
            router,
            jnp.pad(bias_table, (0, own_rows - own_bias))[:, None],
            jnp.zeros((own_rows, spare), jnp.bfloat16),
        ],
        axis=1,
    )
    packed = lax.all_gather(packed, ("dp", "expert"), axis=0, tiled=True)
    packed, (in_shard, down_shard) = tie(packed, (w_in[0], w_down[0]))
    weights = WeightGather(grid, in_shard, down_shard)
    weights.start()
    wqkv = packed[:, : 3 * D]
    wout = packed[:, 3 * D : 4 * D]
    misc = packed[:, 4 * D :]
    gains_f = misc[:, :2].astype(jnp.float32)
    route_w = misc[:, 2 : 2 + experts]
    table = misc[:, 2 + experts].reshape(D // own_rows, own_rows)[:, :own_bias]
    table = table.reshape(BUCKETS, H)

    blocks = rows // LANES + 4
    block_at = jnp.arange(blocks, dtype=jnp.int32)[:, None, None] - 2
    key_at = jnp.arange(LANES, dtype=jnp.int32)[None, :, None]
    query_at = jnp.arange(rows, dtype=jnp.int32)[None, None, :]
    bucket = bucket_of(block_at * LANES + key_at - query_at).reshape(-1)
    bucket_hot = (bucket[None, :] == jnp.arange(BUCKETS, dtype=jnp.int32)[:, None]).astype(
        jnp.bfloat16
    )
    near = jnp.einsum("bh,bn->hn", table, bucket_hot, preferred_element_type=jnp.float32)
    near = near.astype(jnp.bfloat16).reshape(H, blocks, LANES, rows)

    x_rows = tokens.astype(jnp.float32)
    h1 = rms_scale(x_rows, gains_f[:, 0]).astype(jnp.bfloat16)
    qkv = matmul(h1.reshape(micro * rows, D), wqkv)
    qkv = qkv.reshape(micro, rows, 3 * D)
    query = (qkv[..., :D].astype(jnp.bfloat16) * (DH ** (-0.5))).astype(jnp.bfloat16)
    kv_low = qkv[..., D:].astype(jnp.bfloat16)
    starts = []
    for step in range(experts // 2):
        row = (here // 2 + experts // 2 - step) % (experts // 2)
        starts += [(2 * row + here % 2) * rows, (2 * row + 1 - here % 2) * rows]
    metas, kv_pieces, att, lse = [], [], [], []
    for m in range(micro):
        metas.append(jnp.stack([lengths[m, 0], here * rows] + starts).astype(jnp.int32))
        kv_pieces.append(spread(kv_low[m], experts))
    kv_pieces[0], near = weights.finish((kv_pieces[0], near))
    for m in range(micro):
        out, norm = attend(metas[m], query[m], kv_pieces[m], near)
        att.append(out)
        lse.append(norm)
    attended = jnp.stack(att)
    x_mid = x_rows + matmul(attended.reshape(micro * rows, D), wout).reshape(micro, rows, D)
    x_mid = weights.finish(x_mid)
    h2 = rms_scale(x_mid, gains_f[:, 1]).astype(jnp.bfloat16)
    logits = matmul(h2, route_w)
    route_probs = jax.nn.softmax(logits, axis=-1)
    route_hot = (routes[..., None] == jnp.arange(experts, dtype=jnp.int32)).astype(jnp.float32)
    gates = jnp.sum(route_probs[:, :, None, :] * route_hot, axis=-1)
    positions = here * rows + jnp.arange(rows, dtype=jnp.int32)
    live = (positions[None, :] < lengths).astype(jnp.int32)
    slots = jax.vmap(lambda r, l: slot_tables(r, l, experts, capacity))(routes, live)
    columns = jnp.arange(experts * capacity, dtype=jnp.int32)
    hot = [(slots[:, :, j, None] == columns).astype(jnp.bfloat16) for j in range(TOP)]
    any_slot = hot[0] + hot[1]
    sent = jnp.einsum("mts,mtd->msd", any_slot, h2, preferred_element_type=jnp.float32)
    grad_out = cotangent.astype(jnp.float32)
    grad_returned = sum(
        jnp.einsum(
            "mts,mtd->msd",
            hot[j],
            (gates[..., j : j + 1] * grad_out).astype(jnp.bfloat16),
            preferred_element_type=jnp.float32,
        )
        for j in range(TOP)
    )
    both = jnp.concatenate([sent, grad_returned], axis=0).astype(jnp.bfloat16)
    both = weights.finish(swap_slots(both, experts, capacity))
    both, win, wdown = weights.result(both)
    arrived, grad_produced = both[:micro], both[micro:]
    joined = matmul(arrived, win).astype(jnp.bfloat16)
    acted = geglu(joined.astype(jnp.float32)).astype(jnp.bfloat16)
    produced = matmul(acted, wdown).astype(jnp.bfloat16)
    returned = swap_slots(produced, experts, capacity)
    picked = [
        jnp.einsum("mts,msd->mtd", hot[j], returned, preferred_element_type=jnp.float32)
        for j in range(TOP)
    ]
    block_out = x_mid + (gates[..., 0:1] * picked[0] + gates[..., 1:2] * picked[1])
    block_out = block_out.astype(jnp.bfloat16)
    grad_gates = jnp.stack([jnp.sum(grad_out * picked[j], axis=-1) for j in range(TOP)], axis=-1)
    grad_acted = times_trans(grad_produced, wdown)
    grad_joined = jax.vjp(geglu, joined.astype(jnp.float32))[1](grad_acted)[0].astype(jnp.bfloat16)
    grad_arrived = [
        times_trans(grad_joined[m : m + 1], win).astype(jnp.bfloat16) for m in range(micro)
    ]
    grad_arrived, (acted, grad_produced, arrived, grad_joined) = tie(
        grad_arrived, (acted, grad_produced, arrived, grad_joined)
    )
    grad_sent = [swap_slots(part, experts, capacity) for part in grad_arrived]
    sum_down = inner_rows(acted.reshape(-1, FF), grad_produced.reshape(-1, D)).astype(jnp.bfloat16)
    sum_in = inner_rows(arrived.reshape(-1, D), grad_joined.reshape(-1, 2 * FF)).astype(
        jnp.bfloat16
    )
    grad_sent, (sum_down, sum_in) = tie(grad_sent, (sum_down, sum_in))
    grad_sent = jnp.concatenate(grad_sent, axis=0)
    sums = WeightReduce(grid, sum_in, sum_down)
    grad_h2 = jnp.einsum("mts,msd->mtd", any_slot, grad_sent, preferred_element_type=jnp.float32)
    grad_route = jnp.sum(grad_gates[..., None] * route_hot, axis=2)
    grad_logits = route_probs * (
        grad_route - jnp.sum(route_probs * grad_route, axis=-1, keepdims=True)
    )
    grad_logits = grad_logits.astype(jnp.bfloat16)
    sum_router = inner_rows(h2.reshape(-1, D), grad_logits.reshape(-1, experts))
    grad_h2 = grad_h2 + times_trans(grad_logits, route_w)
    grad_mid, grad_gain_two = jax.vjp(rms_scale, x_mid, gains_f[:, 1])[1](grad_h2)
    grad_mid = grad_mid + grad_out
    grad_mid_low = grad_mid.astype(jnp.bfloat16)
    sum_out = inner_rows(attended.reshape(-1, D), grad_mid_low.reshape(-1, D))
    grad_attended = sums.finish(times_trans(grad_mid_low, wout).astype(jnp.bfloat16))
    backs = [
        attend_back(metas[m], query[m], grad_attended[m], att[m], lse[m], kv_pieces[m], near)
        for m in range(micro)
    ]
    backs[-1] = sums.finish(backs[-1])
    near_sum = sum(back[-1] for back in backs)
    grad_query = jnp.stack([back[0] for back in backs])
    grad_kv = []
    for back in backs:
        home = bring_home(back[1:-1], experts).astype(jnp.bfloat16)
        grad_kv.append(jnp.concatenate([home[0], home[1]], axis=1))
    strip_at = jnp.arange(8, dtype=jnp.int32)[None, :, None] + LANES - 8
    column_at = jnp.arange(rows + LANES, dtype=jnp.int32)[None, None, :]
    strip_bucket = bucket_of(block_at * LANES + strip_at - column_at).reshape(-1)
    strip_hot = (strip_bucket[None, :] == jnp.arange(BUCKETS, dtype=jnp.int32)[:, None]).astype(
        jnp.float32
    )
    sum_bias = jnp.einsum(
        "hn,bn->bh", near_sum.reshape(H, -1), strip_hot, precision=lax.Precision.HIGHEST
    )
    sum_query = inner_rows(h1.reshape(-1, D), grad_query.reshape(-1, D)).astype(jnp.bfloat16)
    bias_rows = jnp.pad(
        sum_bias.reshape(D // own_rows, own_bias), ((0, 0), (0, own_rows - own_bias))
    ).reshape(D, 1)
    small = jnp.concatenate(
        [
            sum_query,
            sum_out.astype(jnp.bfloat16),
            grad_gain_two[:, None].astype(jnp.bfloat16),
            sum_router.astype(jnp.bfloat16),
            bias_rows.astype(jnp.bfloat16),
            jnp.zeros((D, LANES - 2 - experts), jnp.bfloat16),
        ],
        axis=1,
    )
    small = Flow(scatter_sum(small, grid, experts))
    grad_kv = advance(sums.finish(jnp.stack(grad_kv)), small)
    sum_kv = inner_rows(h1.reshape(-1, D), grad_kv.reshape(-1, 2 * D)).astype(jnp.bfloat16)
    sum_kv = advance(sum_kv, small)
    late = Flow(scatter_sum(sum_kv, grid, experts))
    grad_qkv = jnp.concatenate([grad_query, grad_kv], axis=2)
    grad_h1 = advance(times_trans(grad_qkv, wqkv), late, small)
    grad_x = jax.vjp(lambda x: rms_scale(x, gains_f[:, 0]), x_rows)[1](grad_h1)[0]
    grad_tokens = advance(grad_x + grad_mid, late, small)
    while late.steps is not None or small.steps is not None:
        advance((), late, small)
    _, out_in, out_down = sums.result(())
    small = small.result
    out_qkv = jnp.concatenate([small[:, :D], late.result], axis=1)
    small = small[:, D:]
    gain_one = jnp.sum(out_qkv * w_qkv.astype(jnp.float32), axis=1) / norm_gains[:, 0].astype(
        jnp.float32
    )
    return (
        block_out,
        grad_tokens,
        out_qkv,
        small[:, :D],
        jnp.stack([gain_one, small[:, D]], axis=1),
        small[:own_bias, D + 1 + experts],
        small[:, D + 1 : D + 1 + experts],
        out_in[None].astype(jnp.float32),
        out_down[None].astype(jnp.float32),
    )


def solution(mesh):
    both = ("dp", "expert")
    in_specs = (
        P(None, both, None),
        P(None, "dp"),
        P(None, both, None),
        P(both, None),
        P(both, None),
        P(both, None),
        P(both),
        P(both, None),
        P("expert", "dp", None),
        P("expert", "dp", None),
        P(None, both, None),
    )
    out_specs = (
        P(None, both, None),
        P(None, both, None),
        P(both, None),
        P(both, None),
        P(both, None),
        P(both),
        P(both, None),
        P("expert", "dp", None),
        P("expert", "dp", None),
    )
    return jax.shard_map(local, mesh=mesh, in_specs=in_specs, out_specs=out_specs, check_vma=False)
```

```python
import jax
import jax.numpy as jnp
from jax import lax
from jax.experimental import pallas as pl
from jax.experimental.pallas import tpu as pltpu
from jax.sharding import PartitionSpec as P

D = 1024
H = 16
DH = 64
FF = 2816
BUCKETS = 32
TOP = 2
PAIRS = H // 2
LANES = 128

bucket_edges = (12, 16, 23, 32, 46, 64, 91)
norm_eps = 1e-06
MASKED = -1e30


def bucket_of(offset):
    dist = jnp.abs(offset)
    beyond = jnp.zeros_like(dist)
    for edge in bucket_edges:
        beyond = beyond + (dist >= edge).astype(jnp.int32)
    near = jnp.where(dist < 8, dist, 8 + beyond)
    return near + 16 * (offset > 0).astype(jnp.int32)


def rms_scale(values, gain):
    return values * lax.rsqrt(jnp.mean(values * values, axis=-1, keepdims=True) + norm_eps) * gain


def geglu(joined):
    half = joined.shape[-1] // 2
    return jax.nn.gelu(joined[..., :half], approximate=True) * joined[..., half:]


def slot_tables(route_rows, live, experts, capacity):
    count, top = route_rows.shape
    picks = (route_rows[:, :, None] == jnp.arange(experts, dtype=jnp.int32)[None, None, :]).astype(
        jnp.int32
    ) * live[:, None, None]
    flat = picks.reshape(count * top, experts)
    before = jnp.cumsum(flat, axis=0) - flat
    place = jnp.sum(before * flat, axis=1).reshape(count, top)
    kept = (place < capacity) & (live[:, None] > 0)
    return jnp.where(kept, route_rows * capacity + place, -1)


def matmul(left, right):
    return jnp.dot(left, right, preferred_element_type=jnp.float32)


def inner_rows(left, right):
    return jnp.einsum("...ti,...tj->ij", left, right, preferred_element_type=jnp.float32)


def times_trans(left, right):
    return jnp.einsum("...ti,ji->...tj", left, right, preferred_element_type=jnp.float32)


def lanes_dot(left, right):
    return lax.dot_general(
        left, right, (((1,), (1,)), ((), ())), preferred_element_type=jnp.float32
    )


def rows_dot(left, right):
    return lax.dot_general(
        left, right, (((0,), (0,)), ((), ())), preferred_element_type=jnp.float32
    )


def block_place(meta_ref, piece, part, blocks):
    place = meta_ref[2 + piece] // LANES + part - meta_ref[1] // LANES + 2
    return jnp.clip(place, 0, blocks - 1)


def attend_kernel(pieces, meta_ref, *refs):
    q_ref, kv_refs, near_ref = refs[0], refs[1 : 1 + 2 * pieces], refs[1 + 2 * pieces]
    att_ref, lse_ref, score_ref = refs[2 + 2 * pieces :]
    k_refs, v_refs = kv_refs[:pieces], kv_refs[pieces:]
    rows = q_ref.shape[0]
    blocks = near_ref.shape[1]
    length = meta_ref[0]
    query = q_ref[...]
    head_of = lax.broadcasted_iota(jnp.int32, (rows, LANES), 1) // DH
    row_head = lax.broadcasted_iota(jnp.int32, (LANES, rows), 0) // DH
    key_row = lax.broadcasted_iota(jnp.int32, (LANES, rows), 0)
    out = None
    for head in range(2):
        own = head_of == head
        query_own = jnp.where(own, query, jnp.zeros_like(query))
        top = jnp.full((1, rows), MASKED, jnp.float32)
        for piece in range(pieces):
            scores = lanes_dot(k_refs[piece][...], query_own)
            for part in range(rows // LANES):
                start = meta_ref[2 + piece] + part * LANES
                block = scores[part * LANES : (part + 1) * LANES]
                block = block + near_ref[head, block_place(meta_ref, piece, part, blocks)].astype(
                    jnp.float32
                )
                block = jnp.where(key_row < length - start, block, MASKED)
                score_ref[pl.ds(piece * rows + part * LANES, LANES), :] = block
                top = jnp.maximum(top, jnp.max(block, axis=0, keepdims=True))
        total = jnp.zeros((LANES, rows), jnp.float32)
        for piece in range(pieces):
            weights = jnp.exp(score_ref[pl.ds(piece * rows, rows), :] - top).astype(jnp.bfloat16)
            value = v_refs[piece][...]
            total = total + rows_dot(jnp.where(own, value, jnp.ones_like(value)), weights)
        other = (1 - head) * DH
        norm = total[other : other + 1]
        lse_ref[0, head : head + 1] = top + jnp.log(norm)
        scaled = total / norm
        out = scaled if out is None else jnp.where(row_head == 0, out, scaled)
    att_ref[...] = out.T.astype(jnp.bfloat16)


def attend_back_kernel(pieces, meta_ref, *refs):
    q_ref, grad_ref, att_ref, lse_ref = refs[:4]
    k_refs, v_refs = refs[4 : 4 + pieces], refs[4 + pieces : 4 + 2 * pieces]
    near_ref = refs[4 + 2 * pieces]
    dq_ref = refs[5 + 2 * pieces]
    dkv_refs = refs[6 + 2 * pieces : 6 + 3 * pieces]
    dnear_ref, block_ref = refs[6 + 3 * pieces :]
    rows = q_ref.shape[0]
    blocks = near_ref.shape[1]
    length = meta_ref[0]
    query = q_ref[...]
    grad = grad_ref[...]
    head_of = lax.broadcasted_iota(jnp.int32, (rows, LANES), 1) // DH
    row_head = lax.broadcasted_iota(jnp.int32, (LANES, rows), 0) // DH
    key_row = lax.broadcasted_iota(jnp.int32, (LANES, rows), 0)
    product = (grad.astype(jnp.float32) * att_ref[...].astype(jnp.float32)).T
    block_ref[...] = jnp.zeros_like(block_ref)
    zero = jnp.zeros_like(query)
    query_own = [jnp.where(head_of == head, query, zero) for head in range(2)]
    grad_own = [jnp.where(head_of == head, grad, zero) for head in range(2)]
    total = [jnp.zeros((LANES, rows), jnp.float32) for head in range(2)]
    delta = [jnp.sum(product[h * DH : (h + 1) * DH], axis=0, keepdims=True) for h in range(2)]
    for piece in range(pieces):
        keys = k_refs[piece][...]
        values = v_refs[piece][...]
        dk = jnp.zeros((rows, LANES), jnp.float32)
        dv = jnp.zeros((rows, LANES), jnp.float32)
        for head in range(2):
            scores = lanes_dot(keys, query_own[head])
            grad_probs = lanes_dot(values, grad_own[head])
            lse = lse_ref[0, head : head + 1]
            prob_parts, ds_parts = [], []
            for part in range(rows // LANES):
                start = meta_ref[2 + piece] + part * LANES
                place = block_place(meta_ref, piece, part, blocks)
                cut = slice(part * LANES, (part + 1) * LANES)
                block = scores[cut] + near_ref[head, place].astype(jnp.float32)
                block = jnp.where(key_row < length - start, block, MASKED)
                probs = jnp.exp(block - lse)
                ds = probs * (grad_probs[cut] - delta[head])
                block_ref[head, place] += ds
                prob_parts.append(probs.astype(jnp.bfloat16))
                ds_parts.append(ds.astype(jnp.bfloat16))
            probs_low = jnp.concatenate(prob_parts, axis=0)
            ds_low = jnp.concatenate(ds_parts, axis=0)
            dv = dv + matmul(probs_low, grad_own[head])
            dk = dk + matmul(ds_low, query_own[head])
            total[head] = total[head] + rows_dot(keys, ds_low)
        dkv_refs[piece][0] = dk.astype(jnp.bfloat16)
        dkv_refs[piece][1] = dv.astype(jnp.bfloat16)
    for head in range(2):
        for place in range(blocks):
            strips = jnp.zeros((8, rows + LANES), jnp.float32)
            for group in range(LANES // 8):
                strip = block_ref[head, place, group * 8 : (group + 1) * 8]
                strip = jnp.concatenate([strip, jnp.zeros((8, LANES), jnp.float32)], axis=1)
                strips = strips + pltpu.roll(strip, LANES - 8 - 8 * group, 1)
            dnear_ref[head, place] = strips
    out = jnp.where(row_head == 0, total[0], total[1])
    dq_ref[...] = (out.T * (DH ** (-0.5))).astype(jnp.bfloat16)


def attend(meta, query, kv_pieces, near):
    rows = query.shape[0]
    pieces = len(kv_pieces)
    blocks = near.shape[1]
    spec = pl.BlockSpec((rows, LANES), lambda i, m: (0, i))
    value_spec = pl.BlockSpec((rows, LANES), lambda i, m: (0, PAIRS + i))
    near_spec = pl.BlockSpec((2, blocks, LANES, rows), lambda i, m: (i, 0, 0, 0))
    lse_spec = pl.BlockSpec((1, 2, rows), lambda i, m: (i, 0, 0))
    flops = 4 * rows * rows * pieces * D
    return pl.pallas_call(
        lambda *refs: attend_kernel(pieces, *refs),
        out_shape=(
            jax.ShapeDtypeStruct((rows, D), jnp.bfloat16),
            jax.ShapeDtypeStruct((PAIRS, 2, rows), jnp.float32),
        ),
        grid_spec=pltpu.PrefetchScalarGridSpec(
            num_scalar_prefetch=1,
            grid=(PAIRS,),
            in_specs=[spec] + [spec] * pieces + [value_spec] * pieces + [near_spec],
            out_specs=[spec, lse_spec],
            scratch_shapes=[pltpu.VMEM((rows * pieces, rows), jnp.float32)],
        ),
        cost_estimate=pl.CostEstimate(
            flops=4 * flops, bytes_accessed=16 * 2**20, transcendentals=rows * rows * pieces * H
        ),
        name="attend",
    )(meta, query, *kv_pieces, *kv_pieces, near)


def attend_back(meta, query, grad, att, lse, kv_pieces, near):
    rows = query.shape[0]
    pieces = len(kv_pieces)
    blocks = near.shape[1]
    spec = pl.BlockSpec((rows, LANES), lambda i, m: (0, i))
    value_spec = pl.BlockSpec((rows, LANES), lambda i, m: (0, PAIRS + i))
    near_spec = pl.BlockSpec((2, blocks, LANES, rows), lambda i, m: (i, 0, 0, 0))
    lse_spec = pl.BlockSpec((1, 2, rows), lambda i, m: (i, 0, 0))
    dkv_spec = pl.BlockSpec((2, rows, LANES), lambda i, m: (0, 0, i))
    flops = 10 * rows * rows * pieces * D
    return pl.pallas_call(
        lambda *refs: attend_back_kernel(pieces, *refs),
        out_shape=(
            [jax.ShapeDtypeStruct((rows, D), jnp.bfloat16)]
            + [jax.ShapeDtypeStruct((2, rows, D), jnp.bfloat16)] * pieces
            + [jax.ShapeDtypeStruct((H, blocks, 8, rows + LANES), jnp.float32)]
        ),
        grid_spec=pltpu.PrefetchScalarGridSpec(
            num_scalar_prefetch=1,
            grid=(PAIRS,),
            in_specs=[spec, spec, spec, lse_spec]
            + [spec] * pieces
            + [value_spec] * pieces
            + [near_spec],
            out_specs=[spec]
            + [dkv_spec] * pieces
            + [pl.BlockSpec((2, blocks, 8, rows + LANES), lambda i, m: (i, 0, 0, 0))],
            scratch_shapes=[pltpu.VMEM((2, blocks, LANES, rows), jnp.float32)],
        ),
        cost_estimate=pl.CostEstimate(
            flops=4 * flops, bytes_accessed=32 * 2**20, transcendentals=rows * rows * pieces * H
        ),
        name="attend_back",
    )(meta, query, grad, att, lse, *kv_pieces, *kv_pieces, near)


def core_swap(values, experts):
    return lax.ppermute(values, "expert", [(e, e ^ 1) for e in range(experts)])


def row_shift(values, experts, step):
    return lax.ppermute(values, "expert", [(e, (e + 2 * step) % experts) for e in range(experts)])


def spread(values, experts):
    pieces = []
    for step in range(experts // 2):
        moved = row_shift(values, experts, step) if step else values
        pieces += [moved, core_swap(moved, experts)]
    return pieces


def bring_home(parts, experts):
    total = None
    for step in range(experts // 2):
        pair = parts[2 * step].astype(jnp.float32) + core_swap(parts[2 * step + 1], experts).astype(
            jnp.float32
        )
        if step:
            pair = row_shift(pair.astype(jnp.bfloat16), experts, -step).astype(jnp.float32)
        total = pair if total is None else total + pair
    return total


class Grid:
    def __init__(self):
        self.columns = lax.axis_size("expert") // 2
        self.rows = lax.axis_size("dp") // self.columns
        self.row = lax.axis_index("dp") // self.columns
        self.column = lax.axis_index("dp") % self.columns

    def shift(self, values, down, right):
        moves = []
        for z in range(self.rows):
            for x in range(self.columns):
                there = (z + down) % self.rows * self.columns + (x + right) % self.columns
                moves.append((z * self.columns + x, there))
        return lax.ppermute(values, "dp", moves)

    def place(self, z, x):
        return (z + self.rows) % self.rows * self.columns + (x + self.columns) % self.columns

    def ring(self, values, sideways):
        chain = [values]
        for _ in range((self.columns if sideways else self.rows) - 1):
            chain.append(self.shift(chain[-1], 0 if sideways else 1, 1 if sideways else 0))
        return chain


def tie(values, transfers):
    return lax.optimization_barrier((values, transfers))


class WeightGather:
    def __init__(self, grid, w_in, w_down):
        many = grid.rows * grid.columns
        self.grid = grid
        self.half = w_down.shape[0] // 2
        self.step = 0
        self.held = [w_in, w_down[: self.half]]
        self.strip = w_down[self.half :]
        self.wgate = jnp.zeros((many, w_in.shape[0], FF), jnp.bfloat16)
        self.wup = jnp.zeros((many, w_in.shape[0], FF), jnp.bfloat16)
        self.wdown = jnp.zeros((many,) + w_down.shape, jnp.bfloat16)

    def start(self):
        grid = self.grid
        last = self.step == grid.rows - 1
        down = None if last else [grid.shift(h, 1, 0) for h in self.held]
        side = [grid.ring(h, True)[1:] for h in self.held]
        if self.step == 0:
            strip = grid.ring(self.strip, True)[1:]
        else:
            strip = grid.shift(self.strip, 1, 0)
        self.moving = (down, side, strip)

    def put(self, x, piece_in, piece_down, half_down, at):
        grid = self.grid
        there = grid.place(grid.row - self.step, grid.column - x)
        if piece_in is not None:
            gate, up = piece_in[None, :, :FF], piece_in[None, :, FF:]
            self.wgate = lax.dynamic_update_slice(self.wgate, gate, (there, 0, 0))
            self.wup = lax.dynamic_update_slice(self.wup, up, (there, 0, 0))
            self.wdown = lax.dynamic_update_slice(self.wdown, piece_down[None], (there, 0, 0))
        if half_down is not None:
            self.wdown = lax.dynamic_update_slice(self.wdown, half_down[None], (there, at, 0))

    def finish(self, values):
        grid = self.grid
        values, (down, side, strip) = tie(values, self.moving)
        if self.step == 0:
            self.strip = jnp.stack([self.strip] + strip)
        else:
            self.strip = strip
        for x in range(grid.columns):
            pieces = self.held if x == 0 else [s[x - 1] for s in side]
            self.put(x, pieces[0], pieces[1], self.strip[x], self.half)
        self.held = down
        self.step += 1
        if self.step < grid.rows:
            self.start()
        return values

    def result(self, values):
        while self.step < self.grid.rows:
            values = self.finish(values)
        gate, up = self.wgate.reshape(D, FF), self.wup.reshape(D, FF)
        return values, gate, up, self.wdown.reshape(FF, D)


class WeightReduce:
    def __init__(self, grid, sum_gate, sum_up, sum_down):
        many = grid.rows * grid.columns
        self.grid = grid
        self.half = FF // many // 2
        self.step = 0
        down = sum_down.reshape(many, FF // many, D)
        self.parts = [
            sum_gate.reshape(many, D // many, FF),
            sum_up.reshape(many, D // many, FF),
            down[:, : self.half],
        ]
        self.strips = down[:, self.half :].reshape(grid.rows, grid.columns, self.half, D)
        self.run = None
        self.strip = self.strip_term(0)
        self.start()

    def term(self, part, x):
        there = self.grid.place(self.grid.row - 1 - self.step, x)
        return lax.dynamic_index_in_dim(part, there, 0, False)

    def strip_term(self, step):
        z = (self.grid.row - 1 - step + self.grid.rows) % self.grid.rows
        return lax.dynamic_index_in_dim(self.strips, z, 0, False)

    def sideways(self, term):
        grid = self.grid
        line = term(grid.column - 1)
        for right in range(1, grid.columns):
            moved = grid.shift(line, 0, 1)
            if right == grid.columns - 1:
                return moved
            line = add_low(moved, term(grid.column - 1 - right))

    def start(self):
        grid = self.grid
        side = [self.sideways(lambda x, p=p: self.term(p, x)) for p in self.parts]
        down = None if self.run is None else [grid.shift(r, 1, 0) for r in self.run]
        if self.step < grid.rows - 1:
            strip = grid.shift(self.strip, 1, 0)
        else:
            strip = self.sideways(self.strip_at)
        self.moving = (side, down, strip)

    def strip_at(self, x):
        x = (x + self.grid.columns) % self.grid.columns
        return lax.dynamic_index_in_dim(self.strip, x, 0, False)

    def finish(self, values):
        grid = self.grid
        values, (self.moving, self.parts) = tie(values, (self.moving, self.parts))
        side, down, strip = self.moving
        lines = []
        for index, part in enumerate(self.parts):
            own = self.term(part, grid.column)
            total = side[index].astype(jnp.float32) + own.astype(jnp.float32)
            if down is not None:
                total = total + down[index].astype(jnp.float32)
            lines.append(total.astype(jnp.bfloat16))
        self.run = lines
        if self.step < grid.rows - 1:
            self.strip = add_low(strip, self.strip_term(self.step + 1))
        else:
            self.strip = add_low(strip, self.strip_at(grid.column))
        self.step += 1
        if self.step < grid.rows:
            self.start()
        return values

    def result(self, values):
        while self.step < self.grid.rows:
            values = self.finish(values)
        joined = jnp.concatenate([self.run[0], self.run[1]], axis=1)
        return values, joined, jnp.concatenate([self.run[2], self.strip], axis=0)


def add_low(left, right):
    return (left.astype(jnp.float32) + right.astype(jnp.float32)).astype(jnp.bfloat16)


class Flow:
    def __init__(self, steps):
        self.steps = steps
        self.result = None
        self.step(None)

    def step(self, landed):
        try:
            self.moving = self.steps.send(landed)
        except StopIteration as end:
            self.result, self.steps, self.moving = end.value, None, None


def advance(values, *flows):
    flows = [flow for flow in flows if flow.steps is not None]
    values, landed = tie(values, [flow.moving for flow in flows])
    for flow, moved in zip(flows, landed):
        flow.step(moved)
    return values


def ring_sum(parts, axis, place, count, shift):
    def term(step):
        return lax.dynamic_index_in_dim(
            parts, (place - 1 - step + 2 * count) % count, axis, False
        )

    run = term(0)
    for step in range(1, count):
        run = add_low((yield shift(run)), term(step))
    return run


def side_by_side(left, right):
    flows = [Flow(left), Flow(right)]
    while any(flow.steps is not None for flow in flows):
        landed = yield [flow.moving for flow in flows]
        for flow, moved in zip(flows, landed):
            if flow.steps is not None:
                flow.step(moved)
    return [flow.result for flow in flows]


def scatter_sum(values, grid, experts):
    lines = experts // 2
    here = lax.axis_index("expert")
    columns = values.shape[1]
    own = values.shape[0] // (grid.rows * grid.columns * experts)
    parts = values.reshape(grid.rows, grid.columns, lines, 2, own, columns)
    parts = yield from ring_sum(parts, 3, here % 2, 2, lambda v: core_swap(v, experts))
    cut = columns // (2 * LANES) * LANES

    def over_y(v, axis):
        return ring_sum(v, axis, here // 2, lines, lambda u: row_shift(u, experts, 1))

    def over_x(v, axis):
        return ring_sum(v, axis, grid.column, grid.columns, lambda u: grid.shift(u, 0, 1))

    def over_z(v):
        return ring_sum(v, 0, grid.row, grid.rows, lambda u: grid.shift(u, 1, 0))

    def left():
        v = yield from over_y(parts[..., :cut], 2)
        v = yield from over_x(v, 1)
        return (yield from over_z(v))

    def right():
        v = yield from over_x(parts[..., cut:], 1)
        v = yield from over_y(v, 1)
        return (yield from over_z(v))

    halves = yield from side_by_side(left(), right())
    return jnp.concatenate(halves, axis=1).astype(jnp.float32)


def swap_slots(values, experts, capacity):
    micro = values.shape[0]
    moved = lax.all_to_all(
        values.reshape(micro, experts, capacity, D),
        "expert",
        split_axis=1,
        concat_axis=1,
        tiled=True,
    )
    return moved.reshape(micro, experts * capacity, D)


def local(
    tokens, lengths, routes, w_qkv, w_out, norm_gains, bias_table, router, w_in, w_down, cotangent
):
    micro, rows, width = tokens.shape
    experts = lax.axis_size("expert")
    here = lax.axis_index("expert")
    capacity = (5 * rows * TOP + 4 * experts - 1) // (4 * experts)
    own_rows = w_qkv.shape[0]
    own_bias = bias_table.shape[0]
    spare = LANES - 3 - experts

    grid = Grid()

    weights = WeightGather(grid, w_in[0], w_down[0])
    weights.start()

    packed = jnp.concatenate(
        [
            w_qkv,
            w_out,
            norm_gains,
            router,
            jnp.pad(bias_table, (0, own_rows - own_bias))[:, None],
            jnp.zeros((own_rows, spare), jnp.bfloat16),
        ],
        axis=1,
    )
    packed = lax.all_gather(packed, ("dp", "expert"), axis=0, tiled=True)
    buffers = (weights.wgate, weights.wup, weights.wdown)
    packed, (weights.wgate, weights.wup, weights.wdown) = tie(packed, buffers)
    wqkv = packed[:, : 3 * D]
    wout = packed[:, 3 * D : 4 * D]
    misc = packed[:, 4 * D :]
    gains_f = misc[:, :2].astype(jnp.float32)
    route_w = misc[:, 2 : 2 + experts]
    table = misc[:, 2 + experts].reshape(D // own_rows, own_rows)[:, :own_bias]
    table = table.reshape(BUCKETS, H)

    blocks = rows // LANES + 4
    block_at = jnp.arange(blocks, dtype=jnp.int32)[:, None, None] - 2
    key_at = jnp.arange(LANES, dtype=jnp.int32)[None, :, None]
    query_at = jnp.arange(rows, dtype=jnp.int32)[None, None, :]
    bucket = bucket_of(block_at * LANES + key_at - query_at).reshape(-1)
    bucket_hot = (bucket[None, :] == jnp.arange(BUCKETS, dtype=jnp.int32)[:, None]).astype(
        jnp.bfloat16
    )
    near = jnp.einsum("bh,bn->hn", table, bucket_hot, preferred_element_type=jnp.float32)
    near = near.astype(jnp.bfloat16).reshape(H, blocks, LANES, rows)

    x_rows = tokens.astype(jnp.float32)
    h1 = rms_scale(x_rows, gains_f[:, 0]).astype(jnp.bfloat16)
    qkv = matmul(h1.reshape(micro * rows, D), wqkv)
    qkv = qkv.reshape(micro, rows, 3 * D)
    query = (qkv[..., :D].astype(jnp.bfloat16) * (DH ** (-0.5))).astype(jnp.bfloat16)
    kv_low = qkv[..., D:].astype(jnp.bfloat16)
    starts = []
    for step in range(experts // 2):
        row = (here // 2 + experts // 2 - step) % (experts // 2)
        starts += [(2 * row + here % 2) * rows, (2 * row + 1 - here % 2) * rows]
    metas, kv_pieces, att, lse = [], [], [], []
    for m in range(micro):
        metas.append(jnp.stack([lengths[m, 0], here * rows] + starts).astype(jnp.int32))
        kv_pieces.append(spread(kv_low[m], experts))
    kv_pieces[0], near = weights.finish((kv_pieces[0], near))
    for m in range(micro):
        out, norm = attend(metas[m], query[m], kv_pieces[m], near)
        att.append(out)
        lse.append(norm)
    attended = jnp.stack(att)
    x_mid = x_rows + matmul(attended.reshape(micro * rows, D), wout).reshape(micro, rows, D)
    x_mid = weights.finish(x_mid)
    h2 = rms_scale(x_mid, gains_f[:, 1]).astype(jnp.bfloat16)
    logits = matmul(h2, route_w)
    route_probs = jax.nn.softmax(logits, axis=-1)
    route_hot = (routes[..., None] == jnp.arange(experts, dtype=jnp.int32)).astype(jnp.float32)
    gates = jnp.sum(route_probs[:, :, None, :] * route_hot, axis=-1)
    positions = here * rows + jnp.arange(rows, dtype=jnp.int32)
    live = (positions[None, :] < lengths).astype(jnp.int32)
    slots = jax.vmap(lambda r, l: slot_tables(r, l, experts, capacity))(routes, live)
    columns = jnp.arange(experts * capacity, dtype=jnp.int32)
    hot = [(slots[:, :, j, None] == columns).astype(jnp.bfloat16) for j in range(TOP)]
    any_slot = hot[0] + hot[1]
    sent = jnp.einsum("mts,mtd->msd", any_slot, h2, preferred_element_type=jnp.float32)
    grad_out = cotangent.astype(jnp.float32)
    grad_returned = sum(
        jnp.einsum(
            "mts,mtd->msd",
            hot[j],
            (gates[..., j : j + 1] * grad_out).astype(jnp.bfloat16),
            preferred_element_type=jnp.float32,
        )
        for j in range(TOP)
    )
    both = jnp.concatenate([sent, grad_returned], axis=0).astype(jnp.bfloat16)
    both = weights.finish(swap_slots(both, experts, capacity))
    both, wgate, wup, wdown = weights.result(both)
    arrived, grad_produced = both[:micro], both[micro:]
    gate_low = lax.optimization_barrier(matmul(arrived, wgate).astype(jnp.bfloat16))
    up_low = lax.optimization_barrier(matmul(arrived, wup).astype(jnp.bfloat16))

    def gelu(values):
        return jax.nn.gelu(values, approximate=True)

    def acted_of(gate, up):
        return (gelu(gate.astype(jnp.float32)) * up.astype(jnp.float32)).astype(jnp.bfloat16)

    acted = lax.optimization_barrier(acted_of(gate_low, up_low))
    produced = matmul(acted, wdown).astype(jnp.bfloat16)
    produced, (gate_low, up_low) = tie(produced, (gate_low, up_low))
    returned = swap_slots(produced, experts, capacity)
    grad_acted = times_trans(grad_produced, wdown)
    gelu_gate, pull_gate = jax.vjp(gelu, gate_low.astype(jnp.float32))
    grad_gate = pull_gate(grad_acted * up_low.astype(jnp.float32))[0].astype(jnp.bfloat16)
    grad_up = (grad_acted * gelu_gate).astype(jnp.bfloat16)
    grad_arrived = [
        (
            times_trans(grad_gate[m : m + 1], wgate) + times_trans(grad_up[m : m + 1], wup)
        ).astype(jnp.bfloat16)
        for m in range(micro)
    ]
    (grad_arrived, returned), (acted, grad_produced, arrived, grad_gate, grad_up) = tie(
        (grad_arrived, returned), (acted, grad_produced, arrived, grad_gate, grad_up)
    )
    grad_sent = [swap_slots(part, experts, capacity) for part in grad_arrived]

    def weight_sum(rows_in, rows_out):
        return inner_rows(
            rows_in.reshape(-1, rows_in.shape[-1]), rows_out.reshape(-1, rows_out.shape[-1])
        ).astype(jnp.bfloat16)

    sum_gate = weight_sum(arrived, grad_gate)
    sum_up = weight_sum(arrived, grad_up)
    sum_down = weight_sum(acted, grad_produced)
    grad_sent, (sum_down, sum_up) = tie(grad_sent, (sum_down, sum_up))
    grad_sent = jnp.concatenate(grad_sent, axis=0)
    sums = WeightReduce(grid, sum_gate, sum_up, sum_down)
    picked = [
        jnp.einsum("mts,msd->mtd", hot[j], returned, preferred_element_type=jnp.float32)
        for j in range(TOP)
    ]
    block_out = x_mid + (gates[..., 0:1] * picked[0] + gates[..., 1:2] * picked[1])
    block_out = block_out.astype(jnp.bfloat16)
    grad_gates = jnp.stack([jnp.sum(grad_out * picked[j], axis=-1) for j in range(TOP)], axis=-1)
    grad_h2 = jnp.einsum("mts,msd->mtd", any_slot, grad_sent, preferred_element_type=jnp.float32)
    grad_route = jnp.sum(grad_gates[..., None] * route_hot, axis=2)
    grad_logits = route_probs * (
        grad_route - jnp.sum(route_probs * grad_route, axis=-1, keepdims=True)
    )
    grad_logits = grad_logits.astype(jnp.bfloat16)
    sum_router = inner_rows(h2.reshape(-1, D), grad_logits.reshape(-1, experts))
    grad_h2 = grad_h2 + times_trans(grad_logits, route_w)
    grad_mid, grad_gain_two = jax.vjp(rms_scale, x_mid, gains_f[:, 1])[1](grad_h2)
    grad_mid = grad_mid + grad_out
    grad_mid_low = grad_mid.astype(jnp.bfloat16)
    sum_out = inner_rows(attended.reshape(-1, D), grad_mid_low.reshape(-1, D))
    grad_attended = sums.finish(times_trans(grad_mid_low, wout).astype(jnp.bfloat16))
    backs = [
        attend_back(metas[m], query[m], grad_attended[m], att[m], lse[m], kv_pieces[m], near)
        for m in range(micro)
    ]
    backs[-1] = sums.finish(backs[-1])
    near_sum = sum(back[-1] for back in backs)
    grad_query = jnp.stack([back[0] for back in backs])
    grad_kv = []
    for back in backs:
        home = bring_home(back[1:-1], experts).astype(jnp.bfloat16)
        grad_kv.append(jnp.concatenate([home[0], home[1]], axis=1))
    strip_at = jnp.arange(8, dtype=jnp.int32)[None, :, None] + LANES - 8
    column_at = jnp.arange(rows + LANES, dtype=jnp.int32)[None, None, :]
    strip_bucket = bucket_of(block_at * LANES + strip_at - column_at).reshape(-1)
    strip_hot = (strip_bucket[None, :] == jnp.arange(BUCKETS, dtype=jnp.int32)[:, None]).astype(
        jnp.float32
    )
    sum_bias = jnp.einsum(
        "hn,bn->bh", near_sum.reshape(H, -1), strip_hot, precision=lax.Precision.HIGHEST
    )
    sum_query = inner_rows(h1.reshape(-1, D), grad_query.reshape(-1, D)).astype(jnp.bfloat16)
    bias_rows = jnp.pad(
        sum_bias.reshape(D // own_rows, own_bias), ((0, 0), (0, own_rows - own_bias))
    ).reshape(D, 1)
    small = jnp.concatenate(
        [
            sum_query,
            sum_out.astype(jnp.bfloat16),
            grad_gain_two[:, None].astype(jnp.bfloat16),
            sum_router.astype(jnp.bfloat16),
            bias_rows.astype(jnp.bfloat16),
            jnp.zeros((D, LANES - 2 - experts), jnp.bfloat16),
        ],
        axis=1,
    )
    small = Flow(scatter_sum(small, grid, experts))
    grad_kv = advance(sums.finish(jnp.stack(grad_kv)), small)
    sum_kv = inner_rows(h1.reshape(-1, D), grad_kv.reshape(-1, 2 * D)).astype(jnp.bfloat16)
    sum_kv = advance(sum_kv, small)
    late = Flow(scatter_sum(sum_kv, grid, experts))
    grad_qkv = jnp.concatenate([grad_query, grad_kv], axis=2)
    grad_h1 = advance(times_trans(grad_qkv, wqkv), late, small)
    grad_x = jax.vjp(lambda x: rms_scale(x, gains_f[:, 0]), x_rows)[1](grad_h1)[0]
    grad_tokens = advance(grad_x + grad_mid, late, small)
    while late.steps is not None or small.steps is not None:
        advance((), late, small)
    _, out_in, out_down = sums.result(())
    small = small.result
    out_qkv = jnp.concatenate([small[:, :D], late.result], axis=1)
    small = small[:, D:]
    gain_one = jnp.sum(out_qkv * w_qkv.astype(jnp.float32), axis=1) / norm_gains[:, 0].astype(
        jnp.float32
    )
    return (
        block_out,
        grad_tokens,
        out_qkv,
        small[:, :D],
        jnp.stack([gain_one, small[:, D]], axis=1),
        small[:own_bias, D + 1 + experts],
        small[:, D + 1 : D + 1 + experts],
        out_in[None].astype(jnp.float32),
        out_down[None].astype(jnp.float32),
    )


def solution(mesh):
    both = ("dp", "expert")
    in_specs = (
        P(None, both, None),
        P(None, "dp"),
        P(None, both, None),
        P(both, None),
        P(both, None),
        P(both, None),
        P(both),
        P(both, None),
        P("expert", "dp", None),
        P("expert", "dp", None),
        P(None, both, None),
    )
    out_specs = (
        P(None, both, None),
        P(None, both, None),
        P(both, None),
        P(both, None),
        P(both, None),
        P(both),
        P(both, None),
        P("expert", "dp", None),
        P("expert", "dp", None),
    )
    return jax.shard_map(local, mesh=mesh, in_specs=in_specs, out_specs=out_specs, check_vma=False)
```

```python
import jax
import jax.numpy as jnp
from jax import lax
from jax.experimental import pallas as pl
from jax.experimental.pallas import tpu as pltpu
from jax.sharding import PartitionSpec as P

D = 1024
H = 16
DH = 64
FF = 2816
BUCKETS = 32
TOP = 2
PAIRS = H // 2
LANES = 128

bucket_edges = (12, 16, 23, 32, 46, 64, 91)
norm_eps = 1e-06
MASKED = -1e30


def bucket_of(offset):
    dist = jnp.abs(offset)
    beyond = jnp.zeros_like(dist)
    for edge in bucket_edges:
        beyond = beyond + (dist >= edge).astype(jnp.int32)
    near = jnp.where(dist < 8, dist, 8 + beyond)
    return near + 16 * (offset > 0).astype(jnp.int32)


def rms_scale(values, gain):
    return values * lax.rsqrt(jnp.mean(values * values, axis=-1, keepdims=True) + norm_eps) * gain


def geglu(joined):
    half = joined.shape[-1] // 2
    return jax.nn.gelu(joined[..., :half], approximate=True) * joined[..., half:]


def slot_tables(route_rows, live, experts, capacity):
    count, top = route_rows.shape
    picks = (route_rows[:, :, None] == jnp.arange(experts, dtype=jnp.int32)[None, None, :]).astype(
        jnp.int32
    ) * live[:, None, None]
    flat = picks.reshape(count * top, experts)
    before = jnp.cumsum(flat, axis=0) - flat
    place = jnp.sum(before * flat, axis=1).reshape(count, top)
    kept = (place < capacity) & (live[:, None] > 0)
    return jnp.where(kept, route_rows * capacity + place, -1)


def matmul(left, right):
    return jnp.dot(left, right, preferred_element_type=jnp.float32)


def inner_rows(left, right):
    return jnp.einsum("...ti,...tj->ij", left, right, preferred_element_type=jnp.float32)


def times_trans(left, right):
    return jnp.einsum("...ti,ji->...tj", left, right, preferred_element_type=jnp.float32)


def lanes_dot(left, right):
    return lax.dot_general(
        left, right, (((1,), (1,)), ((), ())), preferred_element_type=jnp.float32
    )


def rows_dot(left, right):
    return lax.dot_general(
        left, right, (((0,), (0,)), ((), ())), preferred_element_type=jnp.float32
    )


def block_place(meta_ref, piece, part, blocks):
    place = meta_ref[2 + piece] // LANES + part - meta_ref[1] // LANES + 2
    return jnp.clip(place, 0, blocks - 1)


def attend_kernel(pieces, meta_ref, *refs):
    q_ref, kv_refs, near_ref = refs[0], refs[1 : 1 + 2 * pieces], refs[1 + 2 * pieces]
    att_ref, lse_ref, score_ref = refs[2 + 2 * pieces :]
    k_refs, v_refs = kv_refs[:pieces], kv_refs[pieces:]
    rows = q_ref.shape[0]
    blocks = near_ref.shape[1]
    length = meta_ref[0]
    query = q_ref[...]
    head_of = lax.broadcasted_iota(jnp.int32, (rows, LANES), 1) // DH
    row_head = lax.broadcasted_iota(jnp.int32, (LANES, rows), 0) // DH
    key_row = lax.broadcasted_iota(jnp.int32, (LANES, rows), 0)
    out = None
    for head in range(2):
        own = head_of == head
        query_own = jnp.where(own, query, jnp.zeros_like(query))
        top = jnp.full((1, rows), MASKED, jnp.float32)
        for piece in range(pieces):
            scores = lanes_dot(k_refs[piece][...], query_own)
            for part in range(rows // LANES):
                start = meta_ref[2 + piece] + part * LANES
                block = scores[part * LANES : (part + 1) * LANES]
                block = block + near_ref[head, block_place(meta_ref, piece, part, blocks)].astype(
                    jnp.float32
                )
                block = jnp.where(key_row < length - start, block, MASKED)
                score_ref[pl.ds(piece * rows + part * LANES, LANES), :] = block
                top = jnp.maximum(top, jnp.max(block, axis=0, keepdims=True))
        total = jnp.zeros((LANES, rows), jnp.float32)
        for piece in range(pieces):
            weights = jnp.exp(score_ref[pl.ds(piece * rows, rows), :] - top).astype(jnp.bfloat16)
            value = v_refs[piece][...]
            total = total + rows_dot(jnp.where(own, value, jnp.ones_like(value)), weights)
        other = (1 - head) * DH
        norm = total[other : other + 1]
        lse_ref[0, head : head + 1] = top + jnp.log(norm)
        scaled = total / norm
        out = scaled if out is None else jnp.where(row_head == 0, out, scaled)
    att_ref[...] = out.T.astype(jnp.bfloat16)


def attend_back_kernel(pieces, meta_ref, *refs):
    q_ref, grad_ref, att_ref, lse_ref = refs[:4]
    k_refs, v_refs = refs[4 : 4 + pieces], refs[4 + pieces : 4 + 2 * pieces]
    near_ref = refs[4 + 2 * pieces]
    dq_ref = refs[5 + 2 * pieces]
    dkv_refs = refs[6 + 2 * pieces : 6 + 3 * pieces]
    dnear_ref, block_ref = refs[6 + 3 * pieces :]
    rows = q_ref.shape[0]
    blocks = near_ref.shape[1]
    length = meta_ref[0]
    query = q_ref[...]
    grad = grad_ref[...]
    head_of = lax.broadcasted_iota(jnp.int32, (rows, LANES), 1) // DH
    row_head = lax.broadcasted_iota(jnp.int32, (LANES, rows), 0) // DH
    key_row = lax.broadcasted_iota(jnp.int32, (LANES, rows), 0)
    product = (grad.astype(jnp.float32) * att_ref[...].astype(jnp.float32)).T
    block_ref[...] = jnp.zeros_like(block_ref)
    zero = jnp.zeros_like(query)
    query_own = [jnp.where(head_of == head, query, zero) for head in range(2)]
    grad_own = [jnp.where(head_of == head, grad, zero) for head in range(2)]
    total = [jnp.zeros((LANES, rows), jnp.float32) for head in range(2)]
    delta = [jnp.sum(product[h * DH : (h + 1) * DH], axis=0, keepdims=True) for h in range(2)]
    for piece in range(pieces):
        keys = k_refs[piece][...]
        values = v_refs[piece][...]
        dk = jnp.zeros((rows, LANES), jnp.float32)
        dv = jnp.zeros((rows, LANES), jnp.float32)
        for head in range(2):
            scores = lanes_dot(keys, query_own[head])
            grad_probs = lanes_dot(values, grad_own[head])
            lse = lse_ref[0, head : head + 1]
            prob_parts, ds_parts = [], []
            for part in range(rows // LANES):
                start = meta_ref[2 + piece] + part * LANES
                place = block_place(meta_ref, piece, part, blocks)
                cut = slice(part * LANES, (part + 1) * LANES)
                block = scores[cut] + near_ref[head, place].astype(jnp.float32)
                block = jnp.where(key_row < length - start, block, MASKED)
                probs = jnp.exp(block - lse)
                ds = probs * (grad_probs[cut] - delta[head])
                block_ref[head, place] += ds
                prob_parts.append(probs.astype(jnp.bfloat16))
                ds_parts.append(ds.astype(jnp.bfloat16))
            probs_low = jnp.concatenate(prob_parts, axis=0)
            ds_low = jnp.concatenate(ds_parts, axis=0)
            dv = dv + matmul(probs_low, grad_own[head])
            dk = dk + matmul(ds_low, query_own[head])
            total[head] = total[head] + rows_dot(keys, ds_low)
        dkv_refs[piece][0] = dk.astype(jnp.bfloat16)
        dkv_refs[piece][1] = dv.astype(jnp.bfloat16)
    for head in range(2):
        for place in range(blocks):
            strips = jnp.zeros((8, rows + LANES), jnp.float32)
            for group in range(LANES // 8):
                strip = block_ref[head, place, group * 8 : (group + 1) * 8]
                strip = jnp.concatenate([strip, jnp.zeros((8, LANES), jnp.float32)], axis=1)
                strips = strips + pltpu.roll(strip, LANES - 8 - 8 * group, 1)
            dnear_ref[head, place] = strips
    out = jnp.where(row_head == 0, total[0], total[1])
    dq_ref[...] = (out.T * (DH ** (-0.5))).astype(jnp.bfloat16)


def attend(meta, query, kv_pieces, near):
    rows = query.shape[0]
    pieces = len(kv_pieces)
    blocks = near.shape[1]
    spec = pl.BlockSpec((rows, LANES), lambda i, m: (0, i))
    value_spec = pl.BlockSpec((rows, LANES), lambda i, m: (0, PAIRS + i))
    near_spec = pl.BlockSpec((2, blocks, LANES, rows), lambda i, m: (i, 0, 0, 0))
    lse_spec = pl.BlockSpec((1, 2, rows), lambda i, m: (i, 0, 0))
    flops = 4 * rows * rows * pieces * D
    return pl.pallas_call(
        lambda *refs: attend_kernel(pieces, *refs),
        out_shape=(
            jax.ShapeDtypeStruct((rows, D), jnp.bfloat16),
            jax.ShapeDtypeStruct((PAIRS, 2, rows), jnp.float32),
        ),
        grid_spec=pltpu.PrefetchScalarGridSpec(
            num_scalar_prefetch=1,
            grid=(PAIRS,),
            in_specs=[spec] + [spec] * pieces + [value_spec] * pieces + [near_spec],
            out_specs=[spec, lse_spec],
            scratch_shapes=[pltpu.VMEM((rows * pieces, rows), jnp.float32)],
        ),
        cost_estimate=pl.CostEstimate(
            flops=4 * flops, bytes_accessed=16 * 2**20, transcendentals=rows * rows * pieces * H
        ),
        name="attend",
    )(meta, query, *kv_pieces, *kv_pieces, near)


def attend_back(meta, query, grad, att, lse, kv_pieces, near):
    rows = query.shape[0]
    pieces = len(kv_pieces)
    blocks = near.shape[1]
    spec = pl.BlockSpec((rows, LANES), lambda i, m: (0, i))
    value_spec = pl.BlockSpec((rows, LANES), lambda i, m: (0, PAIRS + i))
    near_spec = pl.BlockSpec((2, blocks, LANES, rows), lambda i, m: (i, 0, 0, 0))
    lse_spec = pl.BlockSpec((1, 2, rows), lambda i, m: (i, 0, 0))
    dkv_spec = pl.BlockSpec((2, rows, LANES), lambda i, m: (0, 0, i))
    flops = 10 * rows * rows * pieces * D
    return pl.pallas_call(
        lambda *refs: attend_back_kernel(pieces, *refs),
        out_shape=(
            [jax.ShapeDtypeStruct((rows, D), jnp.bfloat16)]
            + [jax.ShapeDtypeStruct((2, rows, D), jnp.bfloat16)] * pieces
            + [jax.ShapeDtypeStruct((H, blocks, 8, rows + LANES), jnp.float32)]
        ),
        grid_spec=pltpu.PrefetchScalarGridSpec(
            num_scalar_prefetch=1,
            grid=(PAIRS,),
            in_specs=[spec, spec, spec, lse_spec]
            + [spec] * pieces
            + [value_spec] * pieces
            + [near_spec],
            out_specs=[spec]
            + [dkv_spec] * pieces
            + [pl.BlockSpec((2, blocks, 8, rows + LANES), lambda i, m: (i, 0, 0, 0))],
            scratch_shapes=[pltpu.VMEM((2, blocks, LANES, rows), jnp.float32)],
        ),
        cost_estimate=pl.CostEstimate(
            flops=4 * flops, bytes_accessed=32 * 2**20, transcendentals=rows * rows * pieces * H
        ),
        name="attend_back",
    )(meta, query, grad, att, lse, *kv_pieces, *kv_pieces, near)


def core_swap(values, experts):
    return lax.ppermute(values, "expert", [(e, e ^ 1) for e in range(experts)])


def row_shift(values, experts, step):
    return lax.ppermute(values, "expert", [(e, (e + 2 * step) % experts) for e in range(experts)])


def spread(values, experts):
    pieces = []
    for step in range(experts // 2):
        moved = row_shift(values, experts, step) if step else values
        pieces += [moved, core_swap(moved, experts)]
    return pieces


def bring_home(parts, experts):
    total = None
    for step in range(experts // 2):
        pair = parts[2 * step].astype(jnp.float32) + core_swap(parts[2 * step + 1], experts).astype(
            jnp.float32
        )
        if step:
            pair = row_shift(pair.astype(jnp.bfloat16), experts, -step).astype(jnp.float32)
        total = pair if total is None else total + pair
    return total


class Grid:
    def __init__(self):
        self.columns = lax.axis_size("expert") // 2
        self.rows = lax.axis_size("dp") // self.columns
        self.row = lax.axis_index("dp") // self.columns
        self.column = lax.axis_index("dp") % self.columns

    def shift(self, values, down, right):
        moves = []
        for z in range(self.rows):
            for x in range(self.columns):
                there = (z + down) % self.rows * self.columns + (x + right) % self.columns
                moves.append((z * self.columns + x, there))
        return lax.ppermute(values, "dp", moves)

    def place(self, z, x):
        return (z + self.rows) % self.rows * self.columns + (x + self.columns) % self.columns

    def ring(self, values, sideways):
        chain = [values]
        for _ in range((self.columns if sideways else self.rows) - 1):
            chain.append(self.shift(chain[-1], 0 if sideways else 1, 1 if sideways else 0))
        return chain


def tie(values, transfers):
    return lax.optimization_barrier((values, transfers))


class WeightGather:
    def __init__(self, grid, w_in, w_down):
        many = grid.rows * grid.columns
        self.grid = grid
        self.step = 0
        self.held = [w_in, w_down]
        self.found = []
        self.buffers = [
            jnp.zeros((many, w_in.shape[0], FF), jnp.bfloat16),
            jnp.zeros((many, w_in.shape[0], FF), jnp.bfloat16),
            jnp.zeros((many,) + w_down.shape, jnp.bfloat16),
        ]
        self.start()

    def start(self):
        grid = self.grid
        if self.step < grid.rows - 1:
            self.moving = [grid.shift(h, 1, 0) for h in self.held]
        self.found.append([self.held, [grid.ring(h, True)[1:] for h in self.held]])
        self.put(self.step, 0, self.held)

    def finish(self, values):
        if self.step < self.grid.rows - 1:
            values, self.held = tie(values, self.moving)
            self.step += 1
            self.start()
        return values

    def put(self, step, x, pieces):
        grid = self.grid
        at = (grid.place(grid.row - step, grid.column - x), 0, 0)
        parts = [pieces[0][None, :, :FF], pieces[0][None, :, FF:], pieces[1][None]]
        self.buffers = [
            lax.dynamic_update_slice(b, p, at) for b, p in zip(self.buffers, parts)
        ]

    def result(self, values):
        while self.step < self.grid.rows - 1:
            values = self.finish(values)
        for step, (held, side) in enumerate(self.found):
            for x in range(1, self.grid.columns):
                self.put(step, x, [s[x - 1] for s in side])
        gate, up, down = self.buffers
        return values, gate.reshape(D, FF), up.reshape(D, FF), down.reshape(FF, D)


class WeightReduce:
    def __init__(self, grid, sum_gate, sum_up, sum_down):
        many = grid.rows * grid.columns
        self.grid = grid
        self.step = 0
        self.parts = [
            sum_gate.reshape(many, D // many, FF),
            sum_up.reshape(many, D // many, FF),
            sum_down.reshape(many, FF // many, D),
        ]
        self.run = None
        self.side = [self.sideways(0)]
        self.moving = None

    def terms(self, step, x):
        there = self.grid.place(self.grid.row - 1 - step, x)
        gate, up, down = [lax.dynamic_index_in_dim(p, there, 0, False) for p in self.parts]
        return [jnp.concatenate([gate, up], axis=1), down]

    def sideways(self, step):
        grid = self.grid
        lines = self.terms(step, grid.column - 1)
        for right in range(1, grid.columns):
            lines = [grid.shift(line, 0, 1) for line in lines]
            if right < grid.columns - 1:
                own = self.terms(step, grid.column - 1 - right)
                lines = [add_low(line, term) for line, term in zip(lines, own)]
        return lines

    def ahead(self, values):
        if len(self.side) < self.grid.rows:
            values, self.parts = tie(values, self.parts)
            self.side.append(self.sideways(len(self.side)))
        return values

    def finish(self, values):
        grid = self.grid
        step = self.step
        values, (self.moving, self.side[step], self.parts) = tie(
            values, (self.moving, self.side[step], self.parts)
        )
        own = self.terms(step, grid.column)
        run = []
        for index, term in enumerate(own):
            total = self.side[step][index].astype(jnp.float32) + term.astype(jnp.float32)
            if self.moving is not None:
                total = total + self.moving[index].astype(jnp.float32)
            run.append(total.astype(jnp.bfloat16))
        self.run = run
        self.step += 1
        if self.step < grid.rows:
            self.moving = [grid.shift(line, 1, 0) for line in self.run]
            self.run = self.ahead(self.run)
        return values

    def result(self, values):
        while self.step < self.grid.rows:
            values = self.finish(values)
        return values, self.run[0], self.run[1]


def add_low(left, right):
    return (left.astype(jnp.float32) + right.astype(jnp.float32)).astype(jnp.bfloat16)


class Flow:
    def __init__(self, steps):
        self.steps = steps
        self.result = None
        self.step(None)

    def step(self, landed):
        try:
            self.moving = self.steps.send(landed)
        except StopIteration as end:
            self.result, self.steps, self.moving = end.value, None, None


def advance(values, *flows):
    flows = [flow for flow in flows if flow.steps is not None]
    values, landed = tie(values, [flow.moving for flow in flows])
    for flow, moved in zip(flows, landed):
        flow.step(moved)
    return values


def ring_sum(parts, axis, place, count, shift):
    def term(step):
        return lax.dynamic_index_in_dim(
            parts, (place - 1 - step + 2 * count) % count, axis, False
        )

    run = term(0)
    for step in range(1, count):
        run = add_low((yield shift(run)), term(step))
    return run


def side_by_side(left, right):
    flows = [Flow(left), Flow(right)]
    while any(flow.steps is not None for flow in flows):
        landed = yield [flow.moving for flow in flows]
        for flow, moved in zip(flows, landed):
            if flow.steps is not None:
                flow.step(moved)
    return [flow.result for flow in flows]


def scatter_sum(values, grid, experts):
    lines = experts // 2
    here = lax.axis_index("expert")
    columns = values.shape[1]
    own = values.shape[0] // (grid.rows * grid.columns * experts)
    parts = values.reshape(grid.rows, grid.columns, lines, 2, own, columns)
    parts = yield from ring_sum(parts, 3, here % 2, 2, lambda v: core_swap(v, experts))
    cut = columns // (2 * LANES) * LANES

    def over_y(v, axis):
        return ring_sum(v, axis, here // 2, lines, lambda u: row_shift(u, experts, 1))

    def over_x(v, axis):
        return ring_sum(v, axis, grid.column, grid.columns, lambda u: grid.shift(u, 0, 1))

    def over_z(v):
        return ring_sum(v, 0, grid.row, grid.rows, lambda u: grid.shift(u, 1, 0))

    def left():
        v = yield from over_y(parts[..., :cut], 2)
        v = yield from over_x(v, 1)
        return (yield from over_z(v))

    def right():
        v = yield from over_x(parts[..., cut:], 1)
        v = yield from over_y(v, 1)
        return (yield from over_z(v))

    halves = yield from side_by_side(left(), right())
    return jnp.concatenate(halves, axis=1).astype(jnp.float32)


def swap_slots(values, experts, capacity):
    micro = values.shape[0]
    moved = lax.all_to_all(
        values.reshape(micro, experts, capacity, D),
        "expert",
        split_axis=1,
        concat_axis=1,
        tiled=True,
    )
    return moved.reshape(micro, experts * capacity, D)


def local(
    tokens, lengths, routes, w_qkv, w_out, norm_gains, bias_table, router, w_in, w_down, cotangent
):
    micro, rows, width = tokens.shape
    experts = lax.axis_size("expert")
    here = lax.axis_index("expert")
    capacity = (5 * rows * TOP + 4 * experts - 1) // (4 * experts)
    own_rows = w_qkv.shape[0]
    own_bias = bias_table.shape[0]
    spare = LANES - 3 - experts

    grid = Grid()

    weights = WeightGather(grid, w_in[0], w_down[0])

    packed = jnp.concatenate(
        [
            w_qkv,
            w_out,
            norm_gains,
            router,
            jnp.pad(bias_table, (0, own_rows - own_bias))[:, None],
            jnp.zeros((own_rows, spare), jnp.bfloat16),
        ],
        axis=1,
    )
    packed = lax.all_gather(packed, ("dp", "expert"), axis=0, tiled=True)
    packed, weights.buffers = tie(packed, weights.buffers)
    packed = weights.finish(packed)
    wqkv = packed[:, : 3 * D]
    wout = packed[:, 3 * D : 4 * D]
    misc = packed[:, 4 * D :]
    gains_f = misc[:, :2].astype(jnp.float32)
    route_w = misc[:, 2 : 2 + experts]
    table = misc[:, 2 + experts].reshape(D // own_rows, own_rows)[:, :own_bias]
    table = table.reshape(BUCKETS, H)

    blocks = rows // LANES + 4
    block_at = jnp.arange(blocks, dtype=jnp.int32)[:, None, None] - 2
    key_at = jnp.arange(LANES, dtype=jnp.int32)[None, :, None]
    query_at = jnp.arange(rows, dtype=jnp.int32)[None, None, :]
    bucket = bucket_of(block_at * LANES + key_at - query_at).reshape(-1)
    bucket_hot = (bucket[None, :] == jnp.arange(BUCKETS, dtype=jnp.int32)[:, None]).astype(
        jnp.bfloat16
    )
    near = jnp.einsum("bh,bn->hn", table, bucket_hot, preferred_element_type=jnp.float32)
    near = near.astype(jnp.bfloat16).reshape(H, blocks, LANES, rows)

    x_rows = tokens.astype(jnp.float32)
    h1 = rms_scale(x_rows, gains_f[:, 0]).astype(jnp.bfloat16)
    qkv = matmul(h1.reshape(micro * rows, D), wqkv)
    qkv = qkv.reshape(micro, rows, 3 * D)
    query = (qkv[..., :D].astype(jnp.bfloat16) * (DH ** (-0.5))).astype(jnp.bfloat16)
    kv_low = qkv[..., D:].astype(jnp.bfloat16)
    starts = []
    for step in range(experts // 2):
        row = (here // 2 + experts // 2 - step) % (experts // 2)
        starts += [(2 * row + here % 2) * rows, (2 * row + 1 - here % 2) * rows]
    metas, kv_pieces, att, lse = [], [], [], []
    for m in range(micro):
        metas.append(jnp.stack([lengths[m, 0], here * rows] + starts).astype(jnp.int32))
        kv_pieces.append(spread(kv_low[m], experts))
    kv_pieces[0], near = weights.finish((kv_pieces[0], near))
    for m in range(micro):
        out, norm = attend(metas[m], query[m], kv_pieces[m], near)
        att.append(out)
        lse.append(norm)
    attended = jnp.stack(att)
    x_mid = x_rows + matmul(attended.reshape(micro * rows, D), wout).reshape(micro, rows, D)
    x_mid = weights.finish(x_mid)
    h2 = rms_scale(x_mid, gains_f[:, 1]).astype(jnp.bfloat16)
    logits = matmul(h2, route_w)
    route_probs = jax.nn.softmax(logits, axis=-1)
    route_hot = (routes[..., None] == jnp.arange(experts, dtype=jnp.int32)).astype(jnp.float32)
    gates = jnp.sum(route_probs[:, :, None, :] * route_hot, axis=-1)
    positions = here * rows + jnp.arange(rows, dtype=jnp.int32)
    live = (positions[None, :] < lengths).astype(jnp.int32)
    slots = jax.vmap(lambda r, l: slot_tables(r, l, experts, capacity))(routes, live)
    columns = jnp.arange(experts * capacity, dtype=jnp.int32)
    hot = [(slots[:, :, j, None] == columns).astype(jnp.bfloat16) for j in range(TOP)]
    any_slot = hot[0] + hot[1]
    sent = jnp.einsum("mts,mtd->msd", any_slot, h2, preferred_element_type=jnp.float32)
    grad_out = cotangent.astype(jnp.float32)
    grad_returned = sum(
        jnp.einsum(
            "mts,mtd->msd",
            hot[j],
            (gates[..., j : j + 1] * grad_out).astype(jnp.bfloat16),
            preferred_element_type=jnp.float32,
        )
        for j in range(TOP)
    )
    both = jnp.concatenate([sent, grad_returned], axis=0).astype(jnp.bfloat16)
    both = weights.finish(swap_slots(both, experts, capacity))
    both, wgate, wup, wdown = weights.result(both)
    arrived, grad_produced = both[:micro], both[micro:]
    gate_low = lax.optimization_barrier(matmul(arrived, wgate).astype(jnp.bfloat16))
    up_low = lax.optimization_barrier(matmul(arrived, wup).astype(jnp.bfloat16))

    def gelu(values):
        return jax.nn.gelu(values, approximate=True)

    gelu_gate, slope = jax.jvp(
        gelu, (gate_low.astype(jnp.float32),), (jnp.ones(gate_low.shape, jnp.float32),)
    )
    up_wide = up_low.astype(jnp.float32)
    acted, by_up, by_gate = lax.optimization_barrier(
        (
            (gelu_gate * up_wide).astype(jnp.bfloat16),
            gelu_gate.astype(jnp.bfloat16),
            (slope * up_wide).astype(jnp.bfloat16),
        )
    )
    produced = matmul(acted, wdown).astype(jnp.bfloat16)
    produced, (by_up, by_gate) = tie(produced, (by_up, by_gate))
    returned = swap_slots(produced, experts, capacity)
    grad_acted = times_trans(grad_produced, wdown)
    grad_gate = (grad_acted * by_gate.astype(jnp.float32)).astype(jnp.bfloat16)
    grad_up = (grad_acted * by_up.astype(jnp.float32)).astype(jnp.bfloat16)
    grad_arrived = [
        (
            times_trans(grad_gate[m : m + 1], wgate) + times_trans(grad_up[m : m + 1], wup)
        ).astype(jnp.bfloat16)
        for m in range(micro)
    ]
    (grad_arrived, returned), (acted, grad_produced, arrived, grad_gate, grad_up) = tie(
        (grad_arrived, returned), (acted, grad_produced, arrived, grad_gate, grad_up)
    )
    grad_sent = [swap_slots(part, experts, capacity) for part in grad_arrived]

    def weight_sum(rows_in, rows_out):
        return inner_rows(
            rows_in.reshape(-1, rows_in.shape[-1]), rows_out.reshape(-1, rows_out.shape[-1])
        ).astype(jnp.bfloat16)

    sum_gate = weight_sum(arrived, grad_gate)
    sum_up = weight_sum(arrived, grad_up)
    sum_down = weight_sum(acted, grad_produced)
    grad_sent, (sum_down, sum_up) = tie(grad_sent, (sum_down, sum_up))
    grad_sent = jnp.concatenate(grad_sent, axis=0)
    sums = WeightReduce(grid, sum_gate, sum_up, sum_down)
    picked = [
        jnp.einsum("mts,msd->mtd", hot[j], returned, preferred_element_type=jnp.float32)
        for j in range(TOP)
    ]
    block_out = x_mid + (gates[..., 0:1] * picked[0] + gates[..., 1:2] * picked[1])
    block_out = block_out.astype(jnp.bfloat16)
    grad_gates = jnp.stack([jnp.sum(grad_out * picked[j], axis=-1) for j in range(TOP)], axis=-1)
    grad_h2 = jnp.einsum("mts,msd->mtd", any_slot, grad_sent, preferred_element_type=jnp.float32)
    grad_route = jnp.sum(grad_gates[..., None] * route_hot, axis=2)
    grad_logits = route_probs * (
        grad_route - jnp.sum(route_probs * grad_route, axis=-1, keepdims=True)
    )
    grad_logits = grad_logits.astype(jnp.bfloat16)
    sum_router = inner_rows(h2.reshape(-1, D), grad_logits.reshape(-1, experts))
    grad_h2 = grad_h2 + times_trans(grad_logits, route_w)
    grad_mid, grad_gain_two = jax.vjp(rms_scale, x_mid, gains_f[:, 1])[1](grad_h2)
    grad_mid = grad_mid + grad_out
    grad_mid_low = sums.ahead(grad_mid.astype(jnp.bfloat16))
    sum_out = inner_rows(attended.reshape(-1, D), grad_mid_low.reshape(-1, D))
    grad_attended = sums.finish(times_trans(grad_mid_low, wout).astype(jnp.bfloat16))
    backs = [
        attend_back(metas[m], query[m], grad_attended[m], att[m], lse[m], kv_pieces[m], near)
        for m in range(micro)
    ]
    backs[-1] = sums.finish(backs[-1])
    near_sum = sum(back[-1] for back in backs)
    grad_query = jnp.stack([back[0] for back in backs])
    grad_kv = []
    for back in backs:
        home = bring_home(back[1:-1], experts).astype(jnp.bfloat16)
        grad_kv.append(jnp.concatenate([home[0], home[1]], axis=1))
    strip_at = jnp.arange(8, dtype=jnp.int32)[None, :, None] + LANES - 8
    column_at = jnp.arange(rows + LANES, dtype=jnp.int32)[None, None, :]
    strip_bucket = bucket_of(block_at * LANES + strip_at - column_at).reshape(-1)
    strip_hot = (strip_bucket[None, :] == jnp.arange(BUCKETS, dtype=jnp.int32)[:, None]).astype(
        jnp.float32
    )
    sum_bias = jnp.einsum(
        "hn,bn->bh", near_sum.reshape(H, -1), strip_hot, precision=lax.Precision.HIGHEST
    )
    sum_query = inner_rows(h1.reshape(-1, D), grad_query.reshape(-1, D)).astype(jnp.bfloat16)
    bias_rows = jnp.pad(
        sum_bias.reshape(D // own_rows, own_bias), ((0, 0), (0, own_rows - own_bias))
    ).reshape(D, 1)
    small = jnp.concatenate(
        [
            sum_query,
            sum_out.astype(jnp.bfloat16),
            grad_gain_two[:, None].astype(jnp.bfloat16),
            sum_router.astype(jnp.bfloat16),
            bias_rows.astype(jnp.bfloat16),
            jnp.zeros((D, LANES - 2 - experts), jnp.bfloat16),
        ],
        axis=1,
    )
    small = Flow(scatter_sum(small, grid, experts))
    grad_kv = advance(sums.finish(jnp.stack(grad_kv)), small)
    sum_kv = inner_rows(h1.reshape(-1, D), grad_kv.reshape(-1, 2 * D)).astype(jnp.bfloat16)
    sum_kv = advance(sum_kv, small)
    late = Flow(scatter_sum(sum_kv, grid, experts))
    grad_qkv = jnp.concatenate([grad_query, grad_kv], axis=2)
    grad_h1 = advance(times_trans(grad_qkv, wqkv), late, small)
    grad_x = jax.vjp(lambda x: rms_scale(x, gains_f[:, 0]), x_rows)[1](grad_h1)[0]
    grad_tokens = advance(grad_x + grad_mid, late, small)
    while late.steps is not None or small.steps is not None:
        advance((), late, small)
    _, out_in, out_down = sums.result(())
    small = small.result
    out_qkv = jnp.concatenate([small[:, :D], late.result], axis=1)
    small = small[:, D:]
    gain_one = jnp.sum(out_qkv * w_qkv.astype(jnp.float32), axis=1) / norm_gains[:, 0].astype(
        jnp.float32
    )
    return (
        block_out,
        grad_tokens,
        out_qkv,
        small[:, :D],
        jnp.stack([gain_one, small[:, D]], axis=1),
        small[:own_bias, D + 1 + experts],
        small[:, D + 1 : D + 1 + experts],
        out_in[None].astype(jnp.float32),
        out_down[None].astype(jnp.float32),
    )


def solution(mesh):
    both = ("dp", "expert")
    in_specs = (
        P(None, both, None),
        P(None, "dp"),
        P(None, both, None),
        P(both, None),
        P(both, None),
        P(both, None),
        P(both),
        P(both, None),
        P("expert", "dp", None),
        P("expert", "dp", None),
        P(None, both, None),
    )
    out_specs = (
        P(None, both, None),
        P(None, both, None),
        P(both, None),
        P(both, None),
        P(both, None),
        P(both),
        P(both, None),
        P("expert", "dp", None),
        P("expert", "dp", None),
    )
    return jax.shard_map(local, mesh=mesh, in_specs=in_specs, out_specs=out_specs, check_vma=False)
```

```python
import jax
import jax.numpy as jnp
from jax import lax
from jax.experimental import pallas as pl
from jax.experimental.pallas import tpu as pltpu
from jax.sharding import PartitionSpec as P

D = 1024
H = 16
DH = 64
FF = 2816
BUCKETS = 32
TOP = 2
PAIRS = H // 2
LANES = 128

bucket_edges = (12, 16, 23, 32, 46, 64, 91)
norm_eps = 1e-06
MASKED = -1e30


def bucket_of(offset):
    dist = jnp.abs(offset)
    beyond = jnp.zeros_like(dist)
    for edge in bucket_edges:
        beyond = beyond + (dist >= edge).astype(jnp.int32)
    near = jnp.where(dist < 8, dist, 8 + beyond)
    return near + 16 * (offset > 0).astype(jnp.int32)


def rms_scale(values, gain):
    return values * lax.rsqrt(jnp.mean(values * values, axis=-1, keepdims=True) + norm_eps) * gain


def geglu(joined):
    half = joined.shape[-1] // 2
    return jax.nn.gelu(joined[..., :half], approximate=True) * joined[..., half:]


def slot_tables(route_rows, live, experts, capacity):
    count, top = route_rows.shape
    picks = (route_rows[:, :, None] == jnp.arange(experts, dtype=jnp.int32)[None, None, :]).astype(
        jnp.int32
    ) * live[:, None, None]
    flat = picks.reshape(count * top, experts)
    before = jnp.cumsum(flat, axis=0) - flat
    place = jnp.sum(before * flat, axis=1).reshape(count, top)
    kept = (place < capacity) & (live[:, None] > 0)
    return jnp.where(kept, route_rows * capacity + place, -1)


def matmul(left, right):
    return jnp.dot(left, right, preferred_element_type=jnp.float32)


def inner_rows(left, right):
    return jnp.einsum("...ti,...tj->ij", left, right, preferred_element_type=jnp.float32)


def times_trans(left, right):
    return jnp.einsum("...ti,ji->...tj", left, right, preferred_element_type=jnp.float32)


def lanes_dot(left, right):
    return lax.dot_general(
        left, right, (((1,), (1,)), ((), ())), preferred_element_type=jnp.float32
    )


def rows_dot(left, right):
    return lax.dot_general(
        left, right, (((0,), (0,)), ((), ())), preferred_element_type=jnp.float32
    )


def block_place(meta_ref, piece, part, blocks):
    place = meta_ref[2 + piece] // LANES + part - meta_ref[1] // LANES + 2
    return jnp.clip(place, 0, blocks - 1)


def attend_kernel(pieces, meta_ref, *refs):
    q_ref, kv_refs, near_ref = refs[0], refs[1 : 1 + 2 * pieces], refs[1 + 2 * pieces]
    att_ref, lse_ref, score_ref = refs[2 + 2 * pieces :]
    k_refs, v_refs = kv_refs[:pieces], kv_refs[pieces:]
    rows = q_ref.shape[0]
    blocks = near_ref.shape[1]
    length = meta_ref[0]
    query = q_ref[...]
    head_of = lax.broadcasted_iota(jnp.int32, (rows, LANES), 1) // DH
    row_head = lax.broadcasted_iota(jnp.int32, (LANES, rows), 0) // DH
    key_row = lax.broadcasted_iota(jnp.int32, (LANES, rows), 0)
    out = None
    for head in range(2):
        own = head_of == head
        query_own = jnp.where(own, query, jnp.zeros_like(query))
        top = jnp.full((1, rows), MASKED, jnp.float32)
        for piece in range(pieces):
            scores = lanes_dot(k_refs[piece][...], query_own)
            for part in range(rows // LANES):
                start = meta_ref[2 + piece] + part * LANES
                block = scores[part * LANES : (part + 1) * LANES]
                block = block + near_ref[head, block_place(meta_ref, piece, part, blocks)].astype(
                    jnp.float32
                )
                block = jnp.where(key_row < length - start, block, MASKED)
                score_ref[pl.ds(piece * rows + part * LANES, LANES), :] = block
                top = jnp.maximum(top, jnp.max(block, axis=0, keepdims=True))
        total = jnp.zeros((LANES, rows), jnp.float32)
        for piece in range(pieces):
            weights = jnp.exp(score_ref[pl.ds(piece * rows, rows), :] - top).astype(jnp.bfloat16)
            value = v_refs[piece][...]
            total = total + rows_dot(jnp.where(own, value, jnp.ones_like(value)), weights)
        other = (1 - head) * DH
        norm = total[other : other + 1]
        lse_ref[0, head : head + 1] = top + jnp.log(norm)
        scaled = total / norm
        out = scaled if out is None else jnp.where(row_head == 0, out, scaled)
    att_ref[...] = out.T.astype(jnp.bfloat16)


def attend_back_kernel(pieces, meta_ref, *refs):
    q_ref, grad_ref, att_ref, lse_ref = refs[:4]
    k_refs, v_refs = refs[4 : 4 + pieces], refs[4 + pieces : 4 + 2 * pieces]
    near_ref = refs[4 + 2 * pieces]
    dq_ref = refs[5 + 2 * pieces]
    dkv_refs = refs[6 + 2 * pieces : 6 + 3 * pieces]
    dnear_ref, block_ref = refs[6 + 3 * pieces :]
    rows = q_ref.shape[0]
    blocks = near_ref.shape[1]
    length = meta_ref[0]
    query = q_ref[...]
    grad = grad_ref[...]
    head_of = lax.broadcasted_iota(jnp.int32, (rows, LANES), 1) // DH
    row_head = lax.broadcasted_iota(jnp.int32, (LANES, rows), 0) // DH
    key_row = lax.broadcasted_iota(jnp.int32, (LANES, rows), 0)
    product = (grad.astype(jnp.float32) * att_ref[...].astype(jnp.float32)).T
    block_ref[...] = jnp.zeros_like(block_ref)
    zero = jnp.zeros_like(query)
    query_own = [jnp.where(head_of == head, query, zero) for head in range(2)]
    grad_own = [jnp.where(head_of == head, grad, zero) for head in range(2)]
    total = [jnp.zeros((LANES, rows), jnp.float32) for head in range(2)]
    delta = [jnp.sum(product[h * DH : (h + 1) * DH], axis=0, keepdims=True) for h in range(2)]
    for piece in range(pieces):
        keys = k_refs[piece][...]
        values = v_refs[piece][...]
        dk = jnp.zeros((rows, LANES), jnp.float32)
        dv = jnp.zeros((rows, LANES), jnp.float32)
        for head in range(2):
            scores = lanes_dot(keys, query_own[head])
            grad_probs = lanes_dot(values, grad_own[head])
            lse = lse_ref[0, head : head + 1]
            prob_parts, ds_parts = [], []
            for part in range(rows // LANES):
                start = meta_ref[2 + piece] + part * LANES
                place = block_place(meta_ref, piece, part, blocks)
                cut = slice(part * LANES, (part + 1) * LANES)
                block = scores[cut] + near_ref[head, place].astype(jnp.float32)
                block = jnp.where(key_row < length - start, block, MASKED)
                probs = jnp.exp(block - lse)
                ds = probs * (grad_probs[cut] - delta[head])
                block_ref[head, place] += ds
                prob_parts.append(probs.astype(jnp.bfloat16))
                ds_parts.append(ds.astype(jnp.bfloat16))
            probs_low = jnp.concatenate(prob_parts, axis=0)
            ds_low = jnp.concatenate(ds_parts, axis=0)
            dv = dv + matmul(probs_low, grad_own[head])
            dk = dk + matmul(ds_low, query_own[head])
            total[head] = total[head] + rows_dot(keys, ds_low)
        dkv_refs[piece][0] = dk.astype(jnp.bfloat16)
        dkv_refs[piece][1] = dv.astype(jnp.bfloat16)
    for head in range(2):
        for place in range(blocks):
            strips = jnp.zeros((8, rows + LANES), jnp.float32)
            for group in range(LANES // 8):
                strip = block_ref[head, place, group * 8 : (group + 1) * 8]
                strip = jnp.concatenate([strip, jnp.zeros((8, LANES), jnp.float32)], axis=1)
                strips = strips + pltpu.roll(strip, LANES - 8 - 8 * group, 1)
            dnear_ref[head, place] = strips
    out = jnp.where(row_head == 0, total[0], total[1])
    dq_ref[...] = (out.T * (DH ** (-0.5))).astype(jnp.bfloat16)


def attend(meta, query, kv_pieces, near):
    rows = query.shape[0]
    pieces = len(kv_pieces)
    blocks = near.shape[1]
    spec = pl.BlockSpec((rows, LANES), lambda i, m: (0, i))
    value_spec = pl.BlockSpec((rows, LANES), lambda i, m: (0, PAIRS + i))
    near_spec = pl.BlockSpec((2, blocks, LANES, rows), lambda i, m: (i, 0, 0, 0))
    lse_spec = pl.BlockSpec((1, 2, rows), lambda i, m: (i, 0, 0))
    flops = 4 * rows * rows * pieces * D
    return pl.pallas_call(
        lambda *refs: attend_kernel(pieces, *refs),
        out_shape=(
            jax.ShapeDtypeStruct((rows, D), jnp.bfloat16),
            jax.ShapeDtypeStruct((PAIRS, 2, rows), jnp.float32),
        ),
        grid_spec=pltpu.PrefetchScalarGridSpec(
            num_scalar_prefetch=1,
            grid=(PAIRS,),
            in_specs=[spec] + [spec] * pieces + [value_spec] * pieces + [near_spec],
            out_specs=[spec, lse_spec],
            scratch_shapes=[pltpu.VMEM((rows * pieces, rows), jnp.float32)],
        ),
        cost_estimate=pl.CostEstimate(
            flops=4 * flops, bytes_accessed=16 * 2**20, transcendentals=rows * rows * pieces * H
        ),
        name="attend",
    )(meta, query, *kv_pieces, *kv_pieces, near)


def attend_back(meta, query, grad, att, lse, kv_pieces, near):
    rows = query.shape[0]
    pieces = len(kv_pieces)
    blocks = near.shape[1]
    spec = pl.BlockSpec((rows, LANES), lambda i, m: (0, i))
    value_spec = pl.BlockSpec((rows, LANES), lambda i, m: (0, PAIRS + i))
    near_spec = pl.BlockSpec((2, blocks, LANES, rows), lambda i, m: (i, 0, 0, 0))
    lse_spec = pl.BlockSpec((1, 2, rows), lambda i, m: (i, 0, 0))
    dkv_spec = pl.BlockSpec((2, rows, LANES), lambda i, m: (0, 0, i))
    flops = 10 * rows * rows * pieces * D
    return pl.pallas_call(
        lambda *refs: attend_back_kernel(pieces, *refs),
        out_shape=(
            [jax.ShapeDtypeStruct((rows, D), jnp.bfloat16)]
            + [jax.ShapeDtypeStruct((2, rows, D), jnp.bfloat16)] * pieces
            + [jax.ShapeDtypeStruct((H, blocks, 8, rows + LANES), jnp.float32)]
        ),
        grid_spec=pltpu.PrefetchScalarGridSpec(
            num_scalar_prefetch=1,
            grid=(PAIRS,),
            in_specs=[spec, spec, spec, lse_spec]
            + [spec] * pieces
            + [value_spec] * pieces
            + [near_spec],
            out_specs=[spec]
            + [dkv_spec] * pieces
            + [pl.BlockSpec((2, blocks, 8, rows + LANES), lambda i, m: (i, 0, 0, 0))],
            scratch_shapes=[pltpu.VMEM((2, blocks, LANES, rows), jnp.float32)],
        ),
        cost_estimate=pl.CostEstimate(
            flops=4 * flops, bytes_accessed=32 * 2**20, transcendentals=rows * rows * pieces * H
        ),
        name="attend_back",
    )(meta, query, grad, att, lse, *kv_pieces, *kv_pieces, near)


def core_swap(values, experts):
    return lax.ppermute(values, "expert", [(e, e ^ 1) for e in range(experts)])


def row_shift(values, experts, step):
    return lax.ppermute(values, "expert", [(e, (e + 2 * step) % experts) for e in range(experts)])


def spread_rows(values, experts):
    return [row_shift(values, experts, k) if k else values for k in range(experts // 2)]


def spread_cores(rows, experts):
    pieces = []
    for moved in rows:
        pieces += [moved, core_swap(moved, experts)]
    return pieces


def add_cores(parts, experts):
    return [
        add_low(parts[2 * k], core_swap(parts[2 * k + 1], experts)) for k in range(experts // 2)
    ]


def bring_rows(pairs, experts):
    total = pairs[0].astype(jnp.float32)
    for k in range(1, experts // 2):
        total = total + row_shift(pairs[k], experts, -k).astype(jnp.float32)
    return total.astype(jnp.bfloat16)


class Grid:
    def __init__(self):
        self.columns = lax.axis_size("expert") // 2
        self.rows = lax.axis_size("dp") // self.columns
        self.row = lax.axis_index("dp") // self.columns
        self.column = lax.axis_index("dp") % self.columns

    def shift(self, values, down, right):
        moves = []
        for z in range(self.rows):
            for x in range(self.columns):
                there = (z + down) % self.rows * self.columns + (x + right) % self.columns
                moves.append((z * self.columns + x, there))
        return lax.ppermute(values, "dp", moves)

    def place(self, z, x):
        return (z + self.rows) % self.rows * self.columns + (x + self.columns) % self.columns

    def ring(self, values, sideways):
        chain = [values]
        for _ in range((self.columns if sideways else self.rows) - 1):
            chain.append(self.shift(chain[-1], 0 if sideways else 1, 1 if sideways else 0))
        return chain


def tie(values, transfers):
    return lax.optimization_barrier((values, transfers))


class WeightGather:
    def __init__(self, grid, shard, buffers):
        self.grid = grid
        self.step = 0
        self.held = shard
        self.found = []
        self.buffers = buffers
        self.start()

    def start(self):
        grid = self.grid
        if self.step < grid.rows - 1:
            self.moving = grid.shift(self.held, 1, 0)
        self.found.append(grid.ring(self.held, True))
        self.put(self.step, 0)

    def finish(self, values):
        values, self.held = tie(values, self.moving)
        self.step += 1
        self.start()
        return values

    def put(self, step, x):
        grid = self.grid
        at = (grid.place(grid.row - step, grid.column - x), 0, 0)
        piece = self.found[step][x][None]
        begin = 0
        for index, buffer in enumerate(self.buffers):
            part = piece[:, :, begin : begin + buffer.shape[2]]
            self.buffers[index] = lax.dynamic_update_slice(buffer, part, at)
            begin += buffer.shape[2]

    def result(self, values):
        while self.step < self.grid.rows - 1:
            values = self.finish(values)
        for step in range(self.grid.rows):
            for x in range(1, self.grid.columns):
                self.put(step, x)
        return values, [b.reshape(-1, b.shape[2]) for b in self.buffers]


class WeightReduce:
    def __init__(self, grid, *sums):
        many = grid.rows * grid.columns
        self.grid = grid
        self.step = 0
        self.parts = [part.reshape(many, -1, part.shape[1]) for part in sums]
        self.run = None
        self.side = [self.sideways(0)]
        self.moving = None

    def terms(self, step, x):
        there = self.grid.place(self.grid.row - 1 - step, x)
        found = [lax.dynamic_index_in_dim(p, there, 0, False) for p in self.parts]
        return found[0] if len(found) == 1 else jnp.concatenate(found, axis=1)

    def sideways(self, step):
        grid = self.grid
        line = self.terms(step, grid.column - 1)
        for right in range(1, grid.columns):
            line = grid.shift(line, 0, 1)
            if right < grid.columns - 1:
                line = add_low(line, self.terms(step, grid.column - 1 - right))
        return line

    def ahead(self, values):
        if len(self.side) < self.grid.rows:
            values, self.parts = tie(values, self.parts)
            self.side.append(self.sideways(len(self.side)))
        return values

    def finish(self, values):
        grid = self.grid
        step = self.step
        values, (self.moving, self.side[step], self.parts) = tie(
            values, (self.moving, self.side[step], self.parts)
        )
        total = self.side[step].astype(jnp.float32)
        total = total + self.terms(step, grid.column).astype(jnp.float32)
        if self.moving is not None:
            total = total + self.moving.astype(jnp.float32)
        self.run = total.astype(jnp.bfloat16)
        self.step += 1
        if self.step < grid.rows:
            self.moving = grid.shift(self.run, 1, 0)
            self.run = self.ahead(self.run)
        return values

    def result(self, values):
        while self.step < self.grid.rows:
            values = self.finish(values)
        return values, self.run


def add_low(left, right):
    return (left.astype(jnp.float32) + right.astype(jnp.float32)).astype(jnp.bfloat16)


class Flow:
    def __init__(self, steps):
        self.steps = steps
        self.result = None
        self.step(None)

    def step(self, landed):
        try:
            self.moving = self.steps.send(landed)
        except StopIteration as end:
            self.result, self.steps, self.moving = end.value, None, None


def advance(values, *flows):
    flows = [flow for flow in flows if flow.steps is not None]
    values, landed = tie(values, [flow.moving for flow in flows])
    for flow, moved in zip(flows, landed):
        flow.step(moved)
    return values


def ring_sum(parts, axis, place, count, shift):
    def term(step):
        return lax.dynamic_index_in_dim(
            parts, (place - 1 - step + 2 * count) % count, axis, False
        )

    run = term(0)
    for step in range(1, count):
        run = add_low((yield shift(run)), term(step))
    return run


def side_by_side(left, right):
    flows = [Flow(left), Flow(right)]
    while any(flow.steps is not None for flow in flows):
        landed = yield [flow.moving for flow in flows]
        for flow, moved in zip(flows, landed):
            if flow.steps is not None:
                flow.step(moved)
    return [flow.result for flow in flows]


def scatter_sum(values, grid, experts):
    lines = experts // 2
    here = lax.axis_index("expert")
    columns = values.shape[1]
    own = values.shape[0] // (grid.rows * grid.columns * experts)
    parts = values.reshape(grid.rows, grid.columns, lines, 2, own, columns)
    parts = yield from ring_sum(parts, 3, here % 2, 2, lambda v: core_swap(v, experts))
    cut = columns // (2 * LANES) * LANES

    def over_y(v, axis):
        return ring_sum(v, axis, here // 2, lines, lambda u: row_shift(u, experts, 1))

    def over_x(v, axis):
        return ring_sum(v, axis, grid.column, grid.columns, lambda u: grid.shift(u, 0, 1))

    def over_z(v):
        return ring_sum(v, 0, grid.row, grid.rows, lambda u: grid.shift(u, 1, 0))

    def left():
        v = yield from over_y(parts[..., :cut], 2)
        v = yield from over_x(v, 1)
        return (yield from over_z(v))

    def right():
        v = yield from over_x(parts[..., cut:], 1)
        v = yield from over_y(v, 1)
        return (yield from over_z(v))

    halves = yield from side_by_side(left(), right())
    return jnp.concatenate(halves, axis=1).astype(jnp.float32)


def swap_slots(values, experts, capacity):
    micro = values.shape[0]
    moved = lax.all_to_all(
        values.reshape(micro, experts, capacity, D),
        "expert",
        split_axis=1,
        concat_axis=1,
        tiled=True,
    )
    return moved.reshape(micro, experts * capacity, D)


def local(
    tokens, lengths, routes, w_qkv, w_out, norm_gains, bias_table, router, w_in, w_down, cotangent
):
    micro, rows, width = tokens.shape
    experts = lax.axis_size("expert")
    here = lax.axis_index("expert")
    capacity = (5 * rows * TOP + 4 * experts - 1) // (4 * experts)
    own_rows = w_qkv.shape[0]
    own_bias = bias_table.shape[0]
    spare = LANES - 3 - experts

    grid = Grid()

    many = grid.rows * grid.columns
    in_buffers = [jnp.zeros((many, D // many, FF), jnp.bfloat16) for _ in range(2)]
    down_buffers = [jnp.zeros((many, FF // many, D), jnp.bfloat16)]
    into = WeightGather(grid, w_in[0], in_buffers)

    packed = jnp.concatenate(
        [
            w_qkv,
            w_out,
            norm_gains,
            router,
            jnp.pad(bias_table, (0, own_rows - own_bias))[:, None],
            jnp.zeros((own_rows, spare), jnp.bfloat16),
        ],
        axis=1,
    )
    packed = lax.all_gather(packed, ("dp", "expert"), axis=0, tiled=True)
    packed, (into.buffers, down_buffers) = tie(packed, (into.buffers, down_buffers))
    packed = into.finish(packed)
    wqkv = packed[:, : 3 * D]
    wout = packed[:, 3 * D : 4 * D]
    misc = packed[:, 4 * D :]
    gains_f = misc[:, :2].astype(jnp.float32)
    route_w = misc[:, 2 : 2 + experts]
    table = misc[:, 2 + experts].reshape(D // own_rows, own_rows)[:, :own_bias]
    table = table.reshape(BUCKETS, H)

    blocks = rows // LANES + 4
    block_at = jnp.arange(blocks, dtype=jnp.int32)[:, None, None] - 2
    key_at = jnp.arange(LANES, dtype=jnp.int32)[None, :, None]
    query_at = jnp.arange(rows, dtype=jnp.int32)[None, None, :]
    bucket = bucket_of(block_at * LANES + key_at - query_at).reshape(-1)
    bucket_hot = (bucket[None, :] == jnp.arange(BUCKETS, dtype=jnp.int32)[:, None]).astype(
        jnp.bfloat16
    )
    near = jnp.einsum("bh,bn->hn", table, bucket_hot, preferred_element_type=jnp.float32)
    near = near.astype(jnp.bfloat16).reshape(H, blocks, LANES, rows)

    x_rows = tokens.astype(jnp.float32)
    h1 = rms_scale(x_rows, gains_f[:, 0]).astype(jnp.bfloat16)
    qkv = matmul(h1.reshape(micro * rows, D), wqkv).astype(jnp.bfloat16)
    qkv, down_shard = tie(qkv.reshape(micro, rows, 3 * D), w_down[0])
    down = WeightGather(grid, down_shard, down_buffers)
    query = (qkv[..., :D] * (DH ** (-0.5))).astype(jnp.bfloat16)
    kv_low = qkv[..., D:]
    starts = []
    for step in range(experts // 2):
        row = (here // 2 + experts // 2 - step) % (experts // 2)
        starts += [(2 * row + here % 2) * rows, (2 * row + 1 - here % 2) * rows]
    metas = [
        jnp.stack([lengths[m, 0], here * rows] + starts).astype(jnp.int32) for m in range(micro)
    ]
    kv_rows = [spread_rows(kv_low[m], experts) for m in range(micro)]
    kv_pieces, att, lse = [], [], []
    for m in range(micro):
        kv_pieces.append(spread_cores(kv_rows[m], experts))
        if m == 0:
            kv_pieces[0], near = into.finish((kv_pieces[0], near))
        out, norm = attend(metas[m], query[m], kv_pieces[m], near)
        if m + 1 < micro:
            out, kv_rows[m + 1] = tie(out, kv_rows[m + 1])
            out = down.finish(out)
        att.append(out)
        lse.append(norm)
    attended = jnp.stack(att)
    x_mid = x_rows + matmul(attended.reshape(micro * rows, D), wout).reshape(micro, rows, D)
    x_mid = into.finish(x_mid)
    x_mid = down.finish(x_mid)
    h2 = rms_scale(x_mid, gains_f[:, 1]).astype(jnp.bfloat16)
    logits = matmul(h2, route_w)
    route_probs = jax.nn.softmax(logits, axis=-1)
    route_hot = (routes[..., None] == jnp.arange(experts, dtype=jnp.int32)).astype(jnp.float32)
    gates = jnp.sum(route_probs[:, :, None, :] * route_hot, axis=-1)
    positions = here * rows + jnp.arange(rows, dtype=jnp.int32)
    live = (positions[None, :] < lengths).astype(jnp.int32)
    slots = jax.vmap(lambda r, l: slot_tables(r, l, experts, capacity))(routes, live)
    columns = jnp.arange(experts * capacity, dtype=jnp.int32)
    hot = [(slots[:, :, j, None] == columns).astype(jnp.bfloat16) for j in range(TOP)]
    any_slot = hot[0] + hot[1]
    sent = jnp.einsum("mts,mtd->msd", any_slot, h2, preferred_element_type=jnp.float32)
    sent = sent.astype(jnp.bfloat16)
    arrived = swap_slots(sent, experts, capacity)
    sent, gates_low = tie(sent, gates)
    grad_out = cotangent.astype(jnp.float32)
    grad_returned = sum(
        jnp.einsum(
            "mts,mtd->msd",
            hot[j],
            (gates_low[..., j : j + 1] * grad_out).astype(jnp.bfloat16),
            preferred_element_type=jnp.float32,
        )
        for j in range(TOP)
    ).astype(jnp.bfloat16)
    arrived, grad_returned = tie(arrived, grad_returned)
    grad_produced = swap_slots(grad_returned, experts, capacity)
    arrived, (wgate, wup) = into.result(arrived)
    arrived = down.finish(arrived)
    gate_low = lax.optimization_barrier(matmul(arrived, wgate).astype(jnp.bfloat16))
    up_low = lax.optimization_barrier(matmul(arrived, wup).astype(jnp.bfloat16))

    def gelu(values):
        return jax.nn.gelu(values, approximate=True)

    gelu_gate, slope = jax.jvp(
        gelu, (gate_low.astype(jnp.float32),), (jnp.ones(gate_low.shape, jnp.float32),)
    )
    up_wide = up_low.astype(jnp.float32)
    acted, by_up, by_gate = lax.optimization_barrier(
        (
            (gelu_gate * up_wide).astype(jnp.bfloat16),
            gelu_gate.astype(jnp.bfloat16),
            (slope * up_wide).astype(jnp.bfloat16),
        )
    )
    acted, (wdown,) = down.result(acted)
    produced = matmul(acted, wdown).astype(jnp.bfloat16)

    def weight_sum(rows_in, rows_out):
        return inner_rows(
            rows_in.reshape(-1, rows_in.shape[-1]), rows_out.reshape(-1, rows_out.shape[-1])
        ).astype(jnp.bfloat16)

    produced, (acted, grad_produced) = tie(produced, (acted, grad_produced))
    sum_down = weight_sum(acted, grad_produced)
    sum_down, (by_up, by_gate) = tie(sum_down, (by_up, by_gate))
    down_sums = WeightReduce(grid, sum_down)
    returned = swap_slots(produced, experts, capacity)
    grad_acted = times_trans(grad_produced, wdown)
    grad_gate = (grad_acted * by_gate.astype(jnp.float32)).astype(jnp.bfloat16)
    grad_up = (grad_acted * by_up.astype(jnp.float32)).astype(jnp.bfloat16)
    grad_gate, grad_up = down_sums.finish((grad_gate, grad_up))
    grad_arrived = [
        (
            times_trans(grad_gate[m : m + 1], wgate) + times_trans(grad_up[m : m + 1], wup)
        ).astype(jnp.bfloat16)
        for m in range(micro)
    ]
    (grad_arrived, returned), (arrived, grad_gate, grad_up) = tie(
        (grad_arrived, returned), (arrived, grad_gate, grad_up)
    )
    grad_sent = [swap_slots(part, experts, capacity) for part in grad_arrived]
    arrived, grad_gate, grad_up = down_sums.finish((arrived, grad_gate, grad_up))
    sum_gate = weight_sum(arrived, grad_gate)
    sum_gate, (arrived, grad_up) = tie(sum_gate, (arrived, grad_up))
    arrived, grad_up = down_sums.finish((arrived, grad_up))
    sum_up = weight_sum(arrived, grad_up)
    grad_sent, sum_up = tie(grad_sent, sum_up)
    grad_sent = jnp.concatenate(grad_sent, axis=0)
    sums = WeightReduce(grid, sum_gate, sum_up)
    picked = [
        jnp.einsum("mts,msd->mtd", hot[j], returned, preferred_element_type=jnp.float32)
        for j in range(TOP)
    ]
    block_out = x_mid + (gates[..., 0:1] * picked[0] + gates[..., 1:2] * picked[1])
    block_out = block_out.astype(jnp.bfloat16)
    grad_gates = jnp.stack([jnp.sum(grad_out * picked[j], axis=-1) for j in range(TOP)], axis=-1)
    grad_h2 = jnp.einsum("mts,msd->mtd", any_slot, grad_sent, preferred_element_type=jnp.float32)
    grad_route = jnp.sum(grad_gates[..., None] * route_hot, axis=2)
    grad_logits = route_probs * (
        grad_route - jnp.sum(route_probs * grad_route, axis=-1, keepdims=True)
    )
    grad_logits = grad_logits.astype(jnp.bfloat16)
    sum_router = inner_rows(h2.reshape(-1, D), grad_logits.reshape(-1, experts))
    grad_h2 = grad_h2 + times_trans(grad_logits, route_w)
    grad_mid, grad_gain_two = jax.vjp(rms_scale, x_mid, gains_f[:, 1])[1](grad_h2)
    grad_mid = grad_mid + grad_out
    grad_mid_low = sums.ahead(grad_mid.astype(jnp.bfloat16))
    grad_mid_low, out_down = down_sums.result(grad_mid_low)
    sum_out = inner_rows(attended.reshape(-1, D), grad_mid_low.reshape(-1, D))
    grad_attended = sums.finish(times_trans(grad_mid_low, wout).astype(jnp.bfloat16))
    backs = [
        attend_back(metas[m], query[m], grad_attended[m], att[m], lse[m], kv_pieces[m], near)
        for m in range(micro)
    ]
    near_sum = sum(back[-1] for back in backs)
    grad_query = jnp.stack([back[0] for back in backs])
    pairs = [add_cores(back[1:-1], experts) for back in backs]
    pairs[-1], (near_sum, grad_query) = tie(pairs[-1], (near_sum, grad_query))
    homes = [bring_rows(pair, experts) for pair in pairs]
    near_sum, grad_query = sums.finish((near_sum, grad_query))
    grad_kv = [jnp.concatenate([home[0], home[1]], axis=1) for home in homes]
    strip_at = jnp.arange(8, dtype=jnp.int32)[None, :, None] + LANES - 8
    column_at = jnp.arange(rows + LANES, dtype=jnp.int32)[None, None, :]
    strip_bucket = bucket_of(block_at * LANES + strip_at - column_at).reshape(-1)
    strip_hot = (strip_bucket[None, :] == jnp.arange(BUCKETS, dtype=jnp.int32)[:, None]).astype(
        jnp.float32
    )
    sum_bias = jnp.einsum(
        "hn,bn->bh", near_sum.reshape(H, -1), strip_hot, precision=lax.Precision.HIGHEST
    )
    sum_query = inner_rows(h1.reshape(-1, D), grad_query.reshape(-1, D)).astype(jnp.bfloat16)
    bias_rows = jnp.pad(
        sum_bias.reshape(D // own_rows, own_bias), ((0, 0), (0, own_rows - own_bias))
    ).reshape(D, 1)
    small = jnp.concatenate(
        [
            sum_query,
            sum_out.astype(jnp.bfloat16),
            grad_gain_two[:, None].astype(jnp.bfloat16),
            sum_router.astype(jnp.bfloat16),
            bias_rows.astype(jnp.bfloat16),
            jnp.zeros((D, LANES - 2 - experts), jnp.bfloat16),
        ],
        axis=1,
    )
    small = Flow(scatter_sum(small, grid, experts))
    grad_kv = advance(sums.finish(jnp.stack(grad_kv)), small)
    sum_kv = inner_rows(h1.reshape(-1, D), grad_kv.reshape(-1, 2 * D)).astype(jnp.bfloat16)
    sum_kv = advance(sum_kv, small)
    late = Flow(scatter_sum(sum_kv, grid, experts))
    grad_qkv = jnp.concatenate([grad_query, grad_kv], axis=2)
    grad_h1 = advance(times_trans(grad_qkv, wqkv), late, small)
    grad_x = jax.vjp(lambda x: rms_scale(x, gains_f[:, 0]), x_rows)[1](grad_h1)[0]
    grad_tokens = advance(grad_x + grad_mid, late, small)
    while late.steps is not None or small.steps is not None:
        advance((), late, small)
    _, out_in = sums.result(())
    small = small.result
    out_qkv = jnp.concatenate([small[:, :D], late.result], axis=1)
    small = small[:, D:]
    gain_one = jnp.sum(out_qkv * w_qkv.astype(jnp.float32), axis=1) / norm_gains[:, 0].astype(
        jnp.float32
    )
    return (
        block_out,
        grad_tokens,
        out_qkv,
        small[:, :D],
        jnp.stack([gain_one, small[:, D]], axis=1),
        small[:own_bias, D + 1 + experts],
        small[:, D + 1 : D + 1 + experts],
        out_in[None].astype(jnp.float32),
        out_down[None].astype(jnp.float32),
    )


def solution(mesh):
    both = ("dp", "expert")
    in_specs = (
        P(None, both, None),
        P(None, "dp"),
        P(None, both, None),
        P(both, None),
        P(both, None),
        P(both, None),
        P(both),
        P(both, None),
        P("expert", "dp", None),
        P("expert", "dp", None),
        P(None, both, None),
    )
    out_specs = (
        P(None, both, None),
        P(None, both, None),
        P(both, None),
        P(both, None),
        P(both, None),
        P(both),
        P(both, None),
        P("expert", "dp", None),
        P("expert", "dp", None),
    )
    return jax.shard_map(local, mesh=mesh, in_specs=in_specs, out_specs=out_specs, check_vma=False)
```
